512 devices in a mesh: outer: 32 (over y, z_hi, core), inner: 16 (over z_lo, x).
Axes of the slice: x: 4, y: 4, z: 16 (z_hi: 4, z_lo: 4; z = z_hi * 4 + z_lo), core: 2. Of those that a mesh axis runs over, the one named last changes fastest.
Arguments:
- group_latents: bfloat16 [65536, 1024], P(('outer', 'inner')), may hold values from -6 to 6
- slot_ids: int32 [32, 16], P('outer', 'inner'), may hold values from 0 to 15, each once within a row
- slot_embed: bfloat16 [16, 1024], replicated, may hold values from -6 to 6
- merge_latents: bfloat16 [128, 2048], replicated, may hold values from -6 to 6
- query_weight: bfloat16 [2048, 2048], P(None, 'inner'), may hold values from -0.125 to 0.125
- key_weight: bfloat16 [1024, 2048], P(None, 'inner'), may hold values from -0.1875 to 0.1875
- value_weight: bfloat16 [1024, 2048], P(None, 'inner'), may hold values from -0.1875 to 0.1875
- output_weight: bfloat16 [2048, 2048], P('inner'), may hold values from -0.125 to 0.125
- global_latents: bfloat16 [1024, 2048], P(('outer', 'inner')), may hold values from -6 to 6
- decode_query: bfloat16 [2048, 2048], P(None, 'inner'), may hold values from -0.125 to 0.125
- decode_key: bfloat16 [2048, 2048], P(None, 'inner'), may hold values from -0.125 to 0.125
- decode_value: bfloat16 [2048, 2048], P(None, 'inner'), may hold values from -0.125 to 0.125
- decode_output: bfloat16 [2048, 2048], P('inner'), may hold values from -0.125 to 0.125
Outputs:
- decoded: bfloat16 [4096, 2048], P(('outer', 'inner'))
The draws below stay inside these ranges and needn't reach their ends.
Inputs may be any that keep to these rules, and one draw needn't show every extreme that they name: `slot_ids`: each row holds every slot once.
All inputs are finite; a program needn't handle non-finite values.
Results may differ from the reference program's by a relative error of at most 0.014.
Values may be sent and summed in bfloat16 or wider, within the bound.
No kernel may reach another device: no remote copies, remote signals or barrier semaphores. Data moves between devices by JAX's collectives and lax.ppermute only.
A program may use at most 64 MiB of HBM per device.

```python
import jax
import jax.numpy as jnp
from jax import lax

D1 = 1024
D2 = 2048
HEAD = 128
L1 = 128
L2 = 128
G3 = 1024
GROUPS = 512
MERGES = 32
N_OUTER = 32
N_INNER = 16


def block_levels(stream_key, dims, cuts, low, top_value):
    loudness = 1.0
    for position, parts in cuts:
        heights = jax.random.uniform(jax.random.fold_in(jax.random.fold_in(stream_key, 6), position), (parts,), jnp.float32, low / len(cuts), top_value / len(cuts))
        loudness = loudness * jnp.repeat(jnp.exp(heights), dims[position] // parts).reshape((-1,) + (1,) * (len(dims) - 1 - position))
    return loudness


def gaussian(rng, shape, deviation, most, split=(), kind=jnp.bfloat16):
    factor_of = block_levels(rng, shape, split, -0.22, 0.18) if split else 1.0
    drawn = jax.random.normal(rng, shape, jnp.float32) * deviation * factor_of
    return jnp.minimum(jnp.maximum(drawn, -most), most).astype(kind)


def setup_inputs(seed: int = 0) -> dict:
    key_list = jax.random.split(jax.random.key(seed), 14)
    group_latents = gaussian(key_list[0], (GROUPS * L1, D1), 1.0, 6.0, ((0, 512),))
    slot_ids = jax.vmap(lambda own: jax.random.permutation(own, N_INNER))(jax.random.split(key_list[1], MERGES)).reshape((MERGES, N_INNER)).astype(jnp.int32)
    slot_embed = gaussian(key_list[2], (N_INNER, D1), 1.0, 6.0)
    merge_latents = gaussian(key_list[3], (L2, D2), 1.0, 6.0)
    query_weight = gaussian(key_list[4], (D2, D2), D2 ** -0.5, 0.125, ((1, 16),))
    key_weight = gaussian(key_list[5], (D1, D2), D1 ** -0.5, 0.1875, ((1, 16),))
    value_weight = gaussian(key_list[6], (D1, D2), D1 ** -0.5, 0.1875, ((1, 16),))
    output_weight = gaussian(key_list[7], (D2, D2), D2 ** -0.5, 0.125, ((0, 16),))
    global_latents = gaussian(key_list[8], (G3, D2), 1.0, 6.0, ((0, 512),))
    decode_query = gaussian(key_list[9], (D2, D2), D2 ** -0.5, 0.125, ((1, 16),))
    decode_key = gaussian(key_list[10], (D2, D2), D2 ** -0.5, 0.125, ((1, 16),))
    decode_value = gaussian(key_list[11], (D2, D2), D2 ** -0.5, 0.125, ((1, 16),))
    decode_output = gaussian(key_list[12], (D2, D2), D2 ** -0.5, 0.125, ((0, 16),))
    return {"group_latents": group_latents, "slot_ids": slot_ids, "slot_embed": slot_embed, "merge_latents": merge_latents, "query_weight": query_weight, "key_weight": key_weight, "value_weight": value_weight, "output_weight": output_weight, "global_latents": global_latents, "decode_query": decode_query, "decode_key": decode_key, "decode_value": decode_value, "decode_output": decode_output}


def attend(query_rows, key_rows, value_rows):
    length = query_rows.shape[0]
    head_count = query_rows.shape[1] // HEAD
    queries = query_rows.reshape(length, head_count, HEAD).astype(jnp.float32)
    keys_in = key_rows.reshape(key_rows.shape[0], head_count, HEAD).astype(jnp.float32)
    values_in = value_rows.reshape(value_rows.shape[0], head_count, HEAD).astype(jnp.float32)
    scores = jnp.einsum('qhd,khd->hqk', queries, keys_in) * HEAD ** (-0.5)
    weights = jax.nn.softmax(scores, axis=-1).astype(jnp.bfloat16)
    mixed = jnp.einsum('hqk,khd->qhd', weights.astype(jnp.float32), values_in)
    return mixed.reshape(length, head_count * HEAD).astype(jnp.bfloat16)

def reference(group_latents, slot_ids, slot_embed, merge_latents, query_weight, key_weight, value_weight, output_weight, global_latents, decode_query, decode_key, decode_value, decode_output):
    slot_rows = jnp.repeat(slot_embed[slot_ids.reshape(-1)], L1, axis=0)
    keyed = (group_latents.astype(jnp.float32) + slot_rows.astype(jnp.float32)).astype(jnp.bfloat16)
    query_two = jnp.dot(merge_latents, query_weight, preferred_element_type=jnp.float32).astype(jnp.bfloat16)
    key_five = jnp.dot(global_latents, decode_key, preferred_element_type=jnp.float32).astype(jnp.bfloat16)
    value_five = jnp.dot(global_latents, decode_value, preferred_element_type=jnp.float32).astype(jnp.bfloat16)

    def one_merge(merged):
        key_two = jnp.dot(merged, key_weight, preferred_element_type=jnp.float32).astype(jnp.bfloat16)
        value_two = jnp.dot(merged, value_weight, preferred_element_type=jnp.float32).astype(jnp.bfloat16)
        mixed_two = attend(query_two, key_two, value_two)
        level_two = merge_latents.astype(jnp.float32) + jnp.dot(mixed_two, output_weight, preferred_element_type=jnp.float32)
        normed = (level_two * lax.rsqrt(lax.optimization_barrier(jnp.mean(level_two * level_two, axis=-1, keepdims=True)) + 1e-06)).astype(jnp.bfloat16)
        query_five = jnp.dot(normed, decode_query, preferred_element_type=jnp.float32).astype(jnp.bfloat16)
        mixed_five = attend(query_five, key_five, value_five)
        return (level_two + jnp.dot(mixed_five, decode_output, preferred_element_type=jnp.float32)).astype(jnp.bfloat16)
    blocks = keyed.reshape(N_OUTER, N_INNER * L1, D1)
    return lax.map(one_merge, blocks).reshape(N_OUTER * L2, D2)
```

```python
import jax
import jax.numpy as jnp
from jax import lax
from jax.sharding import Mesh
from jax.sharding import PartitionSpec as P

HEAD = 128
AXES = ("y", "h", "c", "z", "x")
INNER = ("z", "x")
OUTER = ("y", "h", "c")
ALL = OUTER + INNER
BF16 = jnp.bfloat16
F32 = jnp.float32
SCALE = HEAD ** (-0.5)


def dot(a, b, dims, kind=F32):
    return lax.dot_general(a, b, (dims, ((), ())), preferred_element_type=kind)


def partner(value, axis, step):
    size = lax.axis_size(axis)
    return lax.ppermute(value, axis, [(i, i ^ step) for i in range(size)])


def all_from(value, axis):
    copies = jnp.broadcast_to(value, (lax.axis_size(axis), *value.shape))
    return lax.all_to_all(copies, axis, split_axis=0, concat_axis=0, tiled=True)


def exchange(tiles, axis):
    return lax.all_to_all(tiles, axis, split_axis=0, concat_axis=0, tiled=True)


def three_parts(value):
    high = lax.reduce_precision(value, 8, 7)
    rest = value - high
    middle = lax.reduce_precision(rest, 8, 7)
    return [part.astype(BF16) for part in (high, middle, rest - middle)]


def local(
    group_latents,
    slot_ids,
    slot_embed,
    merge_latents,
    query_weight,
    key_weight,
    value_weight,
    output_weight,
    global_latents,
    decode_query,
    decode_key,
    decode_value,
    decode_output,
):
    many_x, many_z = lax.axis_size("x"), lax.axis_size("z")
    inner = many_x * many_z
    length, width = merge_latents.shape
    rows = length // inner

    query_two = dot(merge_latents, query_weight, ((1,), (0,))).astype(BF16)
    folded = dot(query_two, key_weight, ((1,), (1,))).astype(BF16)
    head_pack = jnp.concatenate([folded, value_weight.T], axis=0)
    slot_row = lax.dynamic_slice_in_dim(slot_embed, slot_ids[0, 0], 1, 0)
    keyed = (group_latents.astype(F32) + slot_row.astype(F32)).astype(BF16)

    heads = [head_pack]
    blocks = [keyed]
    for step in (2, 3, 1):
        heads.append(partner(head_pack, "x", step))
        blocks.append(partner(keyed, "z", step))
    heads = [heads[0], heads[3], heads[1], heads[2]]

    outer_block = all_from(global_latents, INNER).reshape(-1, width)
    pair_five = jnp.concatenate([decode_key, decode_value], axis=1)
    pairs = dot(outer_block, pair_five, ((1,), (0,))).astype(BF16)
    pairs = all_from(pairs, ("y", "c"))
    many_c = lax.axis_size("c")
    pairs = pairs.reshape(many_c, -1, 2 * HEAD)
    half = lax.dynamic_index_in_dim(pairs, lax.axis_index("c"), 0, keepdims=False)
    half = all_from(half, "h").reshape(-1, 2 * HEAD)
    other = partner(half, "c", 1)

    keys = jnp.concatenate(blocks, axis=0)
    folded_all = jnp.concatenate([pack[:length] for pack in heads], axis=0)
    value_all = jnp.concatenate([pack[length:] for pack in heads], axis=0)
    scores = dot(keys, folded_all, ((1,), (1,))) * SCALE
    values = dot(keys, value_all, ((1,), (1,))).astype(BF16)
    top = jnp.max(scores, axis=0, keepdims=True)
    weights = jnp.exp(scores - top)
    total = jnp.sum(weights, axis=0, keepdims=True)
    level = top + jnp.log(total)
    weights = weights.astype(BF16)
    parts = []
    for k in range(many_x):
        at = slice(k * length, (k + 1) * length)
        of = slice(k * HEAD, (k + 1) * HEAD)
        mixed = dot(values[:, of], weights[:, at], ((0,), (0,))) / total[:, at]
        tail = jnp.concatenate(three_parts(level[:, at]) + [jnp.zeros((5, length), BF16)], axis=0)
        parts.append(jnp.concatenate([mixed.astype(BF16), tail], axis=0))
    parts = jnp.stack(parts)
    mine = lax.axis_index("x")
    places = jnp.arange(many_x, dtype=jnp.int32) ^ mine
    by_place = jnp.take(parts, places, axis=0)
    arrived = exchange(by_place, "x")
    levels = arrived[:, HEAD : HEAD + 3].astype(F32).sum(axis=1, keepdims=True)
    share = jnp.exp(levels - jnp.max(levels, axis=0, keepdims=True))
    share = share / jnp.sum(share, axis=0, keepdims=True)
    mixed_two = jnp.sum(arrived[:, :HEAD].astype(F32) * share, axis=0).astype(BF16)

    partial = dot(mixed_two, output_weight, ((0,), (0,))).astype(BF16)
    arrived = exchange(partial.reshape(inner, rows, width), INNER)
    own = lax.axis_index(INNER) * rows
    own_rows = lax.dynamic_slice_in_dim(merge_latents, own, rows, 0).astype(F32)
    level_two = own_rows + arrived.astype(F32).sum(axis=0)
    normed = (
        level_two * lax.rsqrt(jnp.mean(level_two * level_two, axis=-1, keepdims=True) + 1e-06)
    ).astype(BF16)
    normed = all_from(normed, INNER).reshape(length, width)

    query_five = dot(normed, decode_query, ((1,), (0,))).astype(BF16)
    pairs = jnp.concatenate([half, other], axis=0)
    scores = dot(pairs[:, :HEAD], query_five, ((1,), (1,))) * SCALE
    top = jnp.max(scores, axis=0, keepdims=True)
    weights = jnp.exp(scores - top)
    total = jnp.sum(weights, axis=0, keepdims=True)
    weights = weights.astype(BF16)
    mixed_five = (dot(pairs[:, HEAD:], weights, ((0,), (0,))) / total).astype(BF16)
    partial = dot(mixed_five, decode_output, ((0,), (0,))).astype(BF16)
    arrived = exchange(partial.reshape(inner, rows, width), INNER)
    return (level_two + arrived.astype(F32).sum(axis=0)).astype(BF16)


def solution(mesh):
    outer, inner = mesh.shape["outer"], mesh.shape["inner"]
    finer = Mesh(mesh.devices.reshape(outer // 8, 4, 2, inner // 4, 4), AXES)
    placed = (
        P(ALL, None),
        P(OUTER, INNER),
        P(),
        P(),
        P(None, INNER),
        P(None, INNER),
        P(None, INNER),
        P(INNER, None),
        P(ALL, None),
        P(None, INNER),
        P(None, INNER),
        P(None, INNER),
        P(INNER, None),
    )
    return jax.shard_map(
        local, mesh=finer, in_specs=placed, out_specs=P(ALL, None), check_vma=False
    )
```

```python
import functools

import jax
import jax.numpy as jnp
from jax import lax
from jax.experimental import pallas as pl
from jax.experimental.pallas import tpu as pltpu
from jax.sharding import Mesh
from jax.sharding import PartitionSpec as P


HEAD = 128
AXES = ("y", "h", "c", "z", "x")
INNER = ("z", "x")
OUTER = ("y", "h", "c")
ALL = OUTER + INNER
BF16 = jnp.bfloat16
F32 = jnp.float32
SCALE = HEAD ** (-0.5)
TAIL = 16
PARAMS = pltpu.CompilerParams(vmem_limit_bytes=20 * 2**20)


VMEM = pl.BlockSpec(memory_space=pltpu.VMEM)


def dot(a, b, dims):
    return lax.dot_general(a, b, (dims, ((), ())), preferred_element_type=F32)


def partner(value, axis, step):
    pairs = [(i, i ^ step) for i in range(lax.axis_size(axis))]
    return lax.ppermute(value, axis, pairs)


def exchange(tiles, axis):
    return lax.all_to_all(tiles, axis, split_axis=0, concat_axis=0, tiled=True)


def all_from(value, axis):
    copies = jnp.broadcast_to(value, (lax.axis_size(axis), *value.shape))
    return exchange(copies, axis)


def cost(flops, size):
    return pl.CostEstimate(flops=flops, bytes_accessed=size, transcendentals=0)


def attend_kernel(*refs):
    blocks, packs, out_ref = refs[:4], refs[4:8], refs[8]
    mine = lax.axis_index("x")
    for step, pack_ref in enumerate(packs):
        place = mine ^ step
        pack = pack_ref[...]
        both = [dot(block[...], pack, ((1,), (0,))) for block in blocks]
        scores = jnp.concatenate([b[:, :HEAD] for b in both], axis=0) * SCALE
        values = jnp.concatenate([b[:, HEAD:].astype(BF16) for b in both], axis=0)
        top = jnp.max(scores, axis=0, keepdims=True)
        weights = jnp.exp(scores - top)
        total = jnp.sum(weights, axis=0, keepdims=True)
        mixed = dot(values, weights.astype(BF16), ((0,), (0,))) / total
        level = top + jnp.log(total)
        high = level.astype(BF16).astype(F32)
        middle = (level - high).astype(BF16).astype(F32)
        low = level - high - middle
        line = lax.broadcasted_iota(jnp.int32, (TAIL, mixed.shape[1]), 0)
        tail = jnp.where(line == 0, high, jnp.where(line == 1, middle, jnp.where(line == 2, low, 0.0)))
        out_ref[place] = jnp.concatenate([mixed, tail], axis=0).astype(BF16)


def attend_part(blocks, packs, length):
    many = len(packs)
    keys = sum(b.shape[0] for b in blocks)
    flops = 2 * many * keys * (blocks[0].shape[1] * 2 * HEAD + HEAD * length)
    return pl.pallas_call(
        attend_kernel,
        out_shape=jax.ShapeDtypeStruct((many, HEAD + TAIL, length), BF16),
        in_specs=[VMEM] * (len(blocks) + many),
        out_specs=VMEM,
        compiler_params=PARAMS,
        cost_estimate=cost(flops, 3 * 2**20),
        name="attend_part",
    )(*blocks, *packs)


def join_kernel(parts_ref, weight_ref, out_ref):
    many = parts_ref.shape[0]
    levels = [
        jnp.sum(parts_ref[j, HEAD:, :].astype(F32), axis=0, keepdims=True) for j in range(many)
    ]
    top = functools.reduce(jnp.maximum, levels)
    shares = [jnp.exp(level - top) for level in levels]
    total = functools.reduce(jnp.add, shares)
    mixed = functools.reduce(
        jnp.add, [parts_ref[j, :HEAD, :].astype(F32) * (shares[j] / total) for j in range(many)]
    )
    out_ref[...] = dot(mixed.astype(BF16), weight_ref[...], ((0,), (0,))).astype(BF16)


def join_and_project(parts, weight):
    length, width = parts.shape[2], weight.shape[1]
    return pl.pallas_call(
        join_kernel,
        out_shape=jax.ShapeDtypeStruct((length, width), BF16),
        in_specs=[VMEM, VMEM],
        out_specs=VMEM,
        compiler_params=PARAMS,
        cost_estimate=cost(2 * length * width * HEAD, 2**20),
        name="join_and_project",
    )(parts, weight)


def norm_kernel(parts_ref, own_ref, level_ref, copies_ref):
    many = parts_ref.shape[0]
    level = own_ref[...].astype(F32) + functools.reduce(
        jnp.add, [parts_ref[j].astype(F32) for j in range(many)]
    )
    level_ref[...] = level
    scale = lax.rsqrt(jnp.mean(level * level, axis=-1, keepdims=True) + 1e-06)
    normed = (level * scale).astype(BF16)
    for j in range(many):
        copies_ref[j] = normed


def sum_and_norm(parts, own):
    return pl.pallas_call(
        norm_kernel,
        out_shape=[
            jax.ShapeDtypeStruct(own.shape, F32),
            jax.ShapeDtypeStruct(parts.shape, BF16),
        ],
        in_specs=[VMEM, VMEM],
        out_specs=[VMEM, VMEM],
        compiler_params=PARAMS,
        cost_estimate=cost(4 * parts.size, 2**20),
        name="sum_and_norm",
    )(parts, own)


def last_kernel(parts_ref, level_ref, out_ref):
    total = functools.reduce(
        jnp.add, [parts_ref[j].astype(F32) for j in range(parts_ref.shape[0])]
    )
    out_ref[...] = (level_ref[...] + total).astype(BF16)


def last_sum(parts, level):
    return pl.pallas_call(
        last_kernel,
        out_shape=jax.ShapeDtypeStruct(level.shape, BF16),
        in_specs=[VMEM, VMEM],
        out_specs=VMEM,
        compiler_params=PARAMS,
        cost_estimate=cost(parts.size, 2**20),
        name="last_sum",
    )(parts, level)


def step(
    group_latents,
    slot_ids,
    slot_embed,
    merge_latents,
    query_weight,
    key_weight,
    value_weight,
    output_weight,
    global_latents,
    decode_query,
    decode_key,
    decode_value,
    decode_output,
):
    inner = lax.axis_size(INNER)
    length, width = merge_latents.shape
    rows = length // inner

    query_two = dot(merge_latents, query_weight, ((1,), (0,))).astype(BF16)
    folded = dot(key_weight, query_two, ((1,), (1,))).astype(BF16)
    pack = jnp.concatenate([folded, value_weight], axis=1)
    slot_row = lax.dynamic_slice_in_dim(slot_embed, slot_ids[0, 0], 1, 0)
    keyed = (group_latents.astype(F32) + slot_row.astype(F32)).astype(BF16)
    own_rows = lax.dynamic_slice_in_dim(merge_latents, lax.axis_index(INNER) * rows, rows, 0)

    pack_two = partner(pack, "x", 2)
    keyed_three = partner(keyed, "z", 3)
    outer_block = all_from(global_latents, INNER).reshape(-1, width)
    pack_three = partner(pack, "x", 3)
    keyed_two = partner(keyed, "z", 2)
    pack_one = partner(pack, "x", 1)
    keyed_one = partner(keyed, "z", 1)

    pairs = jnp.concatenate(
        [
            dot(outer_block, decode_key, ((1,), (0,))).astype(BF16),
            dot(outer_block, decode_value, ((1,), (0,))).astype(BF16),
        ],
        axis=1,
    )
    for axis, step_size in (("h", 1), ("h", 2), ("y", 1), ("y", 2)):
        if lax.axis_size(axis) > step_size:
            pairs = jnp.concatenate([pairs, partner(pairs, axis, step_size)], axis=0)
    other = partner(pairs, "c", 1)

    parts = attend_part(
        [keyed, keyed_one, keyed_two, keyed_three],
        [pack, pack_one, pack_two, pack_three],
        length,
    )
    parts = exchange(parts, "x")
    partial = join_and_project(parts, output_weight)
    arrived = exchange(partial.reshape(inner, rows, width), INNER)
    level_two, copies = sum_and_norm(arrived, own_rows)
    normed = exchange(copies, INNER).reshape(length, width)

    query_five = dot(normed, decode_query, ((1,), (0,))).astype(BF16)
    pairs = jnp.concatenate([pairs, other], axis=0)
    scores = dot(pairs[:, :HEAD], query_five, ((1,), (1,))) * SCALE
    top = jnp.max(scores, axis=0, keepdims=True)
    weights = jnp.exp(scores - top)
    total = jnp.sum(weights, axis=0, keepdims=True)
    weights = weights.astype(BF16)
    mixed_five = (dot(pairs[:, HEAD:], weights, ((0,), (0,))) / total).astype(BF16)
    partial = dot(mixed_five, decode_output, ((0,), (0,))).astype(BF16)
    arrived = exchange(partial.reshape(inner, rows, width), INNER)
    return last_sum(arrived, level_two)


def solution(mesh):
    outer, inner = mesh.shape["outer"], mesh.shape["inner"]
    finer = Mesh(mesh.devices.reshape(outer // 8, 4, 2, inner // 4, 4), AXES)
    placed = (
        P(ALL, None),
        P(OUTER, INNER),
        P(),
        P(),
        P(None, INNER),
        P(None, INNER),
        P(None, INNER),
        P(INNER, None),
        P(ALL, None),
        P(None, INNER),
        P(None, INNER),
        P(None, INNER),
        P(INNER, None),
    )
    return jax.shard_map(step, mesh=finer, in_specs=placed, out_specs=P(ALL, None), check_vma=False)
```

```python
import functools

import jax
import jax.numpy as jnp
from jax import lax
from jax.experimental import pallas as pl
from jax.experimental.pallas import tpu as pltpu
from jax.sharding import Mesh
from jax.sharding import PartitionSpec as P


HEAD = 128
AXES = ("y", "h", "c", "z", "x")
INNER = ("z", "x")
OUTER = ("y", "h", "c")
ALL = OUTER + INNER
BF16 = jnp.bfloat16
F32 = jnp.float32
SCALE = HEAD ** (-0.5)
TAIL = 16
EXTRA = 8
PARAMS = pltpu.CompilerParams(vmem_limit_bytes=20 * 2**20)
WIDE = pltpu.CompilerParams(vmem_limit_bytes=62 * 2**20)


VMEM = pl.BlockSpec(memory_space=pltpu.VMEM)


def dot(a, b, dims):
    return lax.dot_general(a, b, (dims, ((), ())), preferred_element_type=F32)


def partner(value, axis, step):
    pairs = [(i, i ^ step) for i in range(lax.axis_size(axis))]
    return lax.ppermute(value, axis, pairs)


def exchange(tiles, axis):
    return lax.all_to_all(tiles, axis, split_axis=0, concat_axis=0, tiled=True)


def cost(flops, size):
    return pl.CostEstimate(flops=flops, bytes_accessed=size, transcendentals=0)


def key_kernel(slot_ref, group_ref, embed_ref, global_ref, out_ref):
    lines = lax.broadcasted_iota(jnp.int32, embed_ref.shape, 0)
    chosen = jnp.where(lines == slot_ref[0, 0], embed_ref[...].astype(F32), 0.0)
    keyed = group_ref[...].astype(F32) + jnp.sum(chosen, axis=0, keepdims=True)
    length, width = group_ref.shape
    latents = global_ref[...].astype(F32)
    rest = jnp.zeros((out_ref.shape[1] - length - 4, width), F32)
    tail = jnp.concatenate([latents[:, :width], latents[:, width:], rest], axis=0)
    block = jnp.concatenate([keyed, tail], axis=0).astype(BF16)
    for j in range(out_ref.shape[0]):
        out_ref[j] = block


def key_copies(slot_ids, group_latents, slot_embed, global_latents, many):
    length, width = group_latents.shape
    return pl.pallas_call(
        key_kernel,
        out_shape=jax.ShapeDtypeStruct((many, length + EXTRA, width), BF16),
        in_specs=[pl.BlockSpec(memory_space=pltpu.SMEM), VMEM, VMEM, VMEM],
        out_specs=VMEM,
        compiler_params=WIDE,
        cost_estimate=cost(4 * group_latents.size, 2**20),
        name="key_copies",
    )(slot_ids, group_latents, slot_embed, global_latents)


def attend_kernel(*refs):
    blocks_ref, packs, out_ref = refs[0], refs[1:-1], refs[-1]
    mine = lax.axis_index("x")
    many, length = blocks_ref.shape[0], blocks_ref.shape[1] - EXTRA
    tails = [blocks_ref[j, length:, :].astype(F32) for j in range(many)]
    latents = jnp.concatenate(
        [
            jnp.concatenate([tail[:2] for tail in tails], axis=0),
            jnp.concatenate([tail[2:4] for tail in tails], axis=0),
        ],
        axis=1,
    )
    pieces = [latents[:, k : k + HEAD] for k in range(0, latents.shape[1], HEAD)]
    for step, pack_ref in enumerate(packs):
        place = mine ^ step
        pack = pack_ref[...]
        both = [dot(blocks_ref[j, :length, :], pack, ((1,), (0,))) for j in range(many)]
        scores = jnp.concatenate([b[:, :-HEAD] for b in both], axis=0) * SCALE
        values = jnp.concatenate([b[:, -HEAD:].astype(BF16) for b in both], axis=0)
        top = jnp.max(scores, axis=0, keepdims=True)
        weights = jnp.exp(scores - top)
        total = jnp.sum(weights, axis=0, keepdims=True)
        mixed = dot(values, weights.astype(BF16), ((0,), (0,))) / total
        level = top + jnp.log(total)
        high = level.astype(BF16).astype(F32)
        middle = (level - high).astype(BF16).astype(F32)
        low = level - high - middle
        line = lax.broadcasted_iota(jnp.int32, (TAIL, mixed.shape[1]), 0)
        tail = jnp.where(line == 0, high, jnp.where(line == 1, middle, jnp.where(line == 2, low, 0.0)))
        out_ref[place] = jnp.concatenate([mixed, tail, *pieces], axis=0).astype(BF16)


def attend_part(blocks, packs):
    many, length = len(packs), packs[0].shape[1] - HEAD
    keys = blocks.shape[0] * blocks.shape[1]
    flops = 2 * many * keys * (blocks.shape[2] * 2 * HEAD + HEAD * length)
    height = HEAD + TAIL + 2 * blocks.shape[0] * 2 * blocks.shape[2] // HEAD
    return pl.pallas_call(
        attend_kernel,
        out_shape=jax.ShapeDtypeStruct((many, height, length), BF16),
        in_specs=[VMEM] * (1 + many),
        out_specs=VMEM,
        compiler_params=WIDE,
        cost_estimate=cost(flops, 3 * 2**20),
        name="attend_part",
    )(blocks, *packs)


def pair_kernel(parts_ref, key_ref, value_ref, out_ref):
    many, height, _ = parts_ref.shape
    lines = []
    for j in range(many):
        pieces = [
            parts_ref[j, k : k + 8, :].astype(F32) for k in range(HEAD + TAIL, height, 8)
        ]
        lines.append(jnp.concatenate(pieces, axis=1))
    latents = jnp.concatenate(lines, axis=0).astype(BF16)
    out_ref[:, :HEAD] = dot(latents, key_ref[...], ((1,), (0,))).astype(BF16)
    out_ref[:, HEAD:] = dot(latents, value_ref[...], ((1,), (0,))).astype(BF16)


def decode_pairs(parts, key_weight, value_weight):
    many, height, length = parts.shape
    size = many * (height - HEAD - TAIL) * length
    rows = size // key_weight.shape[0]
    return pl.pallas_call(
        pair_kernel,
        out_shape=jax.ShapeDtypeStruct((rows, 2 * HEAD), BF16),
        in_specs=[VMEM, VMEM, VMEM],
        out_specs=VMEM,
        compiler_params=PARAMS,
        cost_estimate=cost(4 * size * HEAD, 2**20),
        name="decode_pairs",
    )(parts, key_weight, value_weight)


def join_kernel(parts_ref, weight_ref, out_ref):
    many = parts_ref.shape[0]
    levels = [
        jnp.sum(parts_ref[j, HEAD : HEAD + TAIL, :].astype(F32), axis=0, keepdims=True) for j in range(many)
    ]
    top = functools.reduce(jnp.maximum, levels)
    shares = [jnp.exp(level - top) for level in levels]
    total = functools.reduce(jnp.add, shares)
    mixed = functools.reduce(
        jnp.add, [parts_ref[j, :HEAD, :].astype(F32) * (shares[j] / total) for j in range(many)]
    )
    out_ref[...] = dot(mixed.astype(BF16), weight_ref[...], ((0,), (0,))).astype(BF16)


def join_and_project(parts, weight):
    length, width = parts.shape[2], weight.shape[1]
    return pl.pallas_call(
        join_kernel,
        out_shape=jax.ShapeDtypeStruct((length, width), BF16),
        in_specs=[VMEM, VMEM],
        out_specs=VMEM,
        compiler_params=PARAMS,
        cost_estimate=cost(2 * length * width * HEAD, 2**20),
        name="join_and_project",
    )(parts, weight)


def norm_kernel(parts_ref, own_ref, level_ref, copies_ref):
    many = parts_ref.shape[0]
    level = own_ref[...].astype(F32) + functools.reduce(
        jnp.add, [parts_ref[j].astype(F32) for j in range(many)]
    )
    level_ref[...] = level
    scale = lax.rsqrt(jnp.mean(level * level, axis=-1, keepdims=True) + 1e-06)
    normed = (level * scale).astype(BF16)
    for j in range(many):
        copies_ref[j] = normed


def sum_and_norm(parts, own):
    return pl.pallas_call(
        norm_kernel,
        out_shape=[
            jax.ShapeDtypeStruct(own.shape, F32),
            jax.ShapeDtypeStruct(parts.shape, BF16),
        ],
        in_specs=[VMEM, VMEM],
        out_specs=[VMEM, VMEM],
        compiler_params=PARAMS,
        cost_estimate=cost(4 * parts.size, 2**20),
        name="sum_and_norm",
    )(parts, own)


def last_kernel(parts_ref, level_ref, out_ref):
    total = functools.reduce(
        jnp.add, [parts_ref[j].astype(F32) for j in range(parts_ref.shape[0])]
    )
    out_ref[...] = (level_ref[...] + total).astype(BF16)


def last_sum(parts, level):
    return pl.pallas_call(
        last_kernel,
        out_shape=jax.ShapeDtypeStruct(level.shape, BF16),
        in_specs=[VMEM, VMEM],
        out_specs=VMEM,
        compiler_params=PARAMS,
        cost_estimate=cost(parts.size, 2**20),
        name="last_sum",
    )(parts, level)


def step(
    group_latents,
    slot_ids,
    slot_embed,
    merge_latents,
    query_weight,
    key_weight,
    value_weight,
    output_weight,
    global_latents,
    decode_query,
    decode_key,
    decode_value,
    decode_output,
):
    inner = lax.axis_size(INNER)
    length, width = merge_latents.shape
    rows = length // inner

    query_two = dot(merge_latents, query_weight, ((1,), (0,))).astype(BF16)
    folded = dot(key_weight, query_two, ((1,), (1,))).astype(BF16)
    pack = jnp.concatenate([folded, value_weight], axis=1)
    own_rows = lax.dynamic_slice_in_dim(merge_latents, lax.axis_index(INNER) * rows, rows, 0)

    copies = key_copies(slot_ids, group_latents, slot_embed, global_latents, lax.axis_size("z"))
    blocks = exchange(copies, "z")
    pack_two = partner(pack, "x", 2)
    pack_three = partner(pack, "x", 3)
    pack_one = partner(pack, "x", 1)
    parts = attend_part(blocks, [pack, pack_one, pack_two, pack_three])
    parts = exchange(parts, "x")

    pairs = decode_pairs(parts, decode_key, decode_value)
    for axis, step_size in (("h", 1), ("h", 2), ("y", 1), ("y", 2)):
        if lax.axis_size(axis) > step_size:
            pairs = jnp.concatenate([pairs, partner(pairs, axis, step_size)], axis=0)
    other = partner(pairs, "c", 1)

    partial = join_and_project(parts, output_weight)
    arrived = exchange(partial.reshape(inner, rows, width), INNER)
    level_two, copies = sum_and_norm(arrived, own_rows)
    normed = exchange(copies, INNER).reshape(length, width)

    query_five = dot(normed, decode_query, ((1,), (0,))).astype(BF16)
    pairs = jnp.concatenate([pairs, other], axis=0)
    scores = dot(pairs[:, :HEAD], query_five, ((1,), (1,))) * SCALE
    top = jnp.max(scores, axis=0, keepdims=True)
    weights = jnp.exp(scores - top)
    total = jnp.sum(weights, axis=0, keepdims=True)
    weights = weights.astype(BF16)
    mixed_five = (dot(pairs[:, HEAD:], weights, ((0,), (0,))) / total).astype(BF16)
    partial = dot(mixed_five, decode_output, ((0,), (0,))).astype(BF16)
    arrived = exchange(partial.reshape(inner, rows, width), INNER)
    return last_sum(arrived, level_two)


def solution(mesh):
    outer, inner = mesh.shape["outer"], mesh.shape["inner"]
    finer = Mesh(mesh.devices.reshape(outer // 8, 4, 2, inner // 4, 4), AXES)
    placed = (
        P(ALL, None),
        P(OUTER, INNER),
        P(),
        P(),
        P(None, INNER),
        P(None, INNER),
        P(None, INNER),
        P(INNER, None),
        P(ALL, None),
        P(None, INNER),
        P(None, INNER),
        P(None, INNER),
        P(INNER, None),
    )
    return jax.shard_map(step, mesh=finer, in_specs=placed, out_specs=P(ALL, None), check_vma=False)
```

```python
import functools

import jax
import jax.numpy as jnp
from jax import lax
from jax.experimental import pallas as pl
from jax.experimental.pallas import tpu as pltpu
from jax.sharding import Mesh
from jax.sharding import PartitionSpec as P


HEAD = 128
AXES = ("y", "h", "c", "z", "x")
INNER = ("z", "x")
OUTER = ("y", "h", "c")
ALL = OUTER + INNER
BF16 = jnp.bfloat16
F32 = jnp.float32
SCALE = HEAD ** (-0.5)
TAIL = 16
PARAMS = pltpu.CompilerParams(vmem_limit_bytes=20 * 2**20)
WIDE = pltpu.CompilerParams(vmem_limit_bytes=62 * 2**20)


VMEM = pl.BlockSpec(memory_space=pltpu.VMEM)


def dot(a, b, dims):
    return lax.dot_general(a, b, (dims, ((), ())), preferred_element_type=F32)


def partner(value, axis, step):
    pairs = [(i, i ^ step) for i in range(lax.axis_size(axis))]
    return lax.ppermute(value, axis, pairs)


def exchange(tiles, axis):
    return lax.all_to_all(tiles, axis, split_axis=0, concat_axis=0, tiled=True)


def all_from(value, axis):
    copies = jnp.broadcast_to(value, (lax.axis_size(axis), *value.shape))
    return exchange(copies, axis)


def cost(flops, size):
    return pl.CostEstimate(flops=flops, bytes_accessed=size, transcendentals=0)


def key_kernel(slot_ref, group_ref, embed_ref, out_ref):
    lines = lax.broadcasted_iota(jnp.int32, embed_ref.shape, 0)
    chosen = jnp.where(lines == slot_ref[0, 0], embed_ref[...].astype(F32), 0.0)
    keyed = group_ref[...].astype(F32) + jnp.sum(chosen, axis=0, keepdims=True)
    block = keyed.astype(BF16)
    for j in range(out_ref.shape[0]):
        out_ref[j] = block


def key_copies(slot_ids, group_latents, slot_embed, many):
    return pl.pallas_call(
        key_kernel,
        out_shape=jax.ShapeDtypeStruct((many, *group_latents.shape), BF16),
        in_specs=[pl.BlockSpec(memory_space=pltpu.SMEM), VMEM, VMEM],
        out_specs=VMEM,
        compiler_params=WIDE,
        cost_estimate=cost(4 * group_latents.size, 2**20),
        name="key_copies",
    )(slot_ids, group_latents, slot_embed)


def attend_one(blocks_ref, pack):
    many = blocks_ref.shape[0]
    both = [dot(blocks_ref[j], pack, ((1,), (0,))) for j in range(many)]
    scores = jnp.concatenate([b[:, :-HEAD] for b in both], axis=0) * SCALE
    values = jnp.concatenate([b[:, -HEAD:].astype(BF16) for b in both], axis=0)
    top = jnp.max(scores, axis=0, keepdims=True)
    weights = jnp.exp(scores - top)
    total = jnp.sum(weights, axis=0, keepdims=True)
    mixed = dot(values, weights.astype(BF16), ((0,), (0,))) / total
    level = top + jnp.log(total)
    high = level.astype(BF16).astype(F32)
    middle = (level - high).astype(BF16).astype(F32)
    low = level - high - middle
    line = lax.broadcasted_iota(jnp.int32, (TAIL, mixed.shape[1]), 0)
    tail = jnp.where(line == 0, high, jnp.where(line == 1, middle, jnp.where(line == 2, low, 0.0)))
    return jnp.concatenate([mixed, tail], axis=0).astype(BF16)


def first_kernel(blocks_ref, *refs):
    out_ref = refs[-1]
    for k, pack_ref in enumerate(refs[:-1]):
        out_ref[k] = attend_one(blocks_ref, pack_ref[...])


def second_kernel(steps, blocks_ref, done_ref, *refs):
    out_ref = refs[-1]
    mine = lax.axis_index("x")
    for k in range(done_ref.shape[0]):
        out_ref[mine ^ steps[k]] = done_ref[k]
    for k, pack_ref in enumerate(refs[:-1]):
        out_ref[mine ^ steps[done_ref.shape[0] + k]] = attend_one(blocks_ref, pack_ref[...])


def attend_part(blocks, packs, done=None, steps=None):
    length = packs[0].shape[1] - HEAD
    many = len(packs) + (0 if done is None else done.shape[0])
    keys = blocks.shape[0] * blocks.shape[1]
    flops = 2 * len(packs) * keys * (blocks.shape[2] * 2 * HEAD + HEAD * length)
    given = [blocks] if done is None else [blocks, done]
    return pl.pallas_call(
        first_kernel if done is None else functools.partial(second_kernel, steps),
        out_shape=jax.ShapeDtypeStruct((many, HEAD + TAIL, length), BF16),
        in_specs=[VMEM] * (len(given) + len(packs)),
        out_specs=VMEM,
        compiler_params=WIDE,
        cost_estimate=cost(flops, 3 * 2**20),
        name="attend_first" if done is None else "attend_second",
    )(*given, *packs)


def pair_kernel(parts_ref, key_ref, value_ref, out_ref):
    lines = [parts_ref[j].astype(F32) for j in range(parts_ref.shape[0])]
    latents = jnp.concatenate(lines, axis=0).astype(BF16)
    out_ref[:, :HEAD] = dot(latents, key_ref[...], ((1,), (0,))).astype(BF16)
    out_ref[:, HEAD:] = dot(latents, value_ref[...], ((1,), (0,))).astype(BF16)


def decode_pairs(parts, key_weight, value_weight):
    rows = parts.shape[0] * parts.shape[1]
    return pl.pallas_call(
        pair_kernel,
        out_shape=jax.ShapeDtypeStruct((rows, 2 * HEAD), BF16),
        in_specs=[VMEM, VMEM, VMEM],
        out_specs=VMEM,
        compiler_params=PARAMS,
        cost_estimate=cost(4 * parts.size * HEAD, 2**20),
        name="decode_pairs",
    )(parts, key_weight, value_weight)


def join_kernel(parts_ref, weight_ref, out_ref):
    many = parts_ref.shape[0]
    levels = [
        jnp.sum(parts_ref[j, HEAD : HEAD + TAIL, :].astype(F32), axis=0, keepdims=True) for j in range(many)
    ]
    top = functools.reduce(jnp.maximum, levels)
    shares = [jnp.exp(level - top) for level in levels]
    total = functools.reduce(jnp.add, shares)
    mixed = functools.reduce(
        jnp.add, [parts_ref[j, :HEAD, :].astype(F32) * (shares[j] / total) for j in range(many)]
    )
    out_ref[...] = dot(mixed.astype(BF16), weight_ref[...], ((0,), (0,))).astype(BF16)


def join_and_project(parts, weight):
    length, width = parts.shape[2], weight.shape[1]
    return pl.pallas_call(
        join_kernel,
        out_shape=jax.ShapeDtypeStruct((length, width), BF16),
        in_specs=[VMEM, VMEM],
        out_specs=VMEM,
        compiler_params=PARAMS,
        cost_estimate=cost(2 * length * width * HEAD, 2**20),
        name="join_and_project",
    )(parts, weight)


def norm_kernel(parts_ref, own_ref, level_ref, copies_ref):
    many = parts_ref.shape[0]
    level = own_ref[...].astype(F32) + functools.reduce(
        jnp.add, [parts_ref[j].astype(F32) for j in range(many)]
    )
    level_ref[...] = level
    scale = lax.rsqrt(jnp.mean(level * level, axis=-1, keepdims=True) + 1e-06)
    normed = (level * scale).astype(BF16)
    for j in range(many):
        copies_ref[j] = normed


def sum_and_norm(parts, own):
    return pl.pallas_call(
        norm_kernel,
        out_shape=[
            jax.ShapeDtypeStruct(own.shape, F32),
            jax.ShapeDtypeStruct(parts.shape, BF16),
        ],
        in_specs=[VMEM, VMEM],
        out_specs=[VMEM, VMEM],
        compiler_params=PARAMS,
        cost_estimate=cost(4 * parts.size, 2**20),
        name="sum_and_norm",
    )(parts, own)


def last_kernel(parts_ref, level_ref, out_ref):
    total = functools.reduce(
        jnp.add, [parts_ref[j].astype(F32) for j in range(parts_ref.shape[0])]
    )
    out_ref[...] = (level_ref[...] + total).astype(BF16)


def last_sum(parts, level):
    return pl.pallas_call(
        last_kernel,
        out_shape=jax.ShapeDtypeStruct(level.shape, BF16),
        in_specs=[VMEM, VMEM],
        out_specs=VMEM,
        compiler_params=PARAMS,
        cost_estimate=cost(parts.size, 2**20),
        name="last_sum",
    )(parts, level)


def step(
    group_latents,
    slot_ids,
    slot_embed,
    merge_latents,
    query_weight,
    key_weight,
    value_weight,
    output_weight,
    global_latents,
    decode_query,
    decode_key,
    decode_value,
    decode_output,
):
    inner = lax.axis_size(INNER)
    length, width = merge_latents.shape
    rows = length // inner

    query_two = dot(merge_latents, query_weight, ((1,), (0,))).astype(BF16)
    folded = dot(key_weight, query_two, ((1,), (1,))).astype(BF16)
    pack = jnp.concatenate([folded, value_weight], axis=1)
    own_rows = lax.dynamic_slice_in_dim(merge_latents, lax.axis_index(INNER) * rows, rows, 0)

    copies = key_copies(slot_ids, group_latents, slot_embed, lax.axis_size("z"))
    blocks = exchange(copies, "z")
    pack_two = partner(pack, "x", 2)
    pack_three = partner(pack, "x", 3)
    pack_one = partner(pack, "x", 1)
    done = attend_part(blocks, [pack, pack_two])
    outer_block = all_from(global_latents, INNER)
    parts = attend_part(blocks, [pack_three, pack_one], done, (0, 2, 3, 1))
    parts = exchange(parts, "x")

    pairs = decode_pairs(outer_block, decode_key, decode_value)
    for axis, step_size in (("h", 1), ("h", 3), ("y", 1), ("y", 3)):
        if lax.axis_size(axis) > step_size:
            pairs = jnp.concatenate([pairs, partner(pairs, axis, step_size)], axis=0)
    other = partner(pairs, "c", 1)

    partial = join_and_project(parts, output_weight)
    arrived = exchange(partial.reshape(inner, rows, width), INNER)
    level_two, copies = sum_and_norm(arrived, own_rows)
    normed = exchange(copies, INNER).reshape(length, width)

    query_five = dot(normed, decode_query, ((1,), (0,))).astype(BF16)
    pairs = jnp.concatenate([pairs, other], axis=0)
    scores = dot(pairs[:, :HEAD], query_five, ((1,), (1,))) * SCALE
    top = jnp.max(scores, axis=0, keepdims=True)
    weights = jnp.exp(scores - top)
    total = jnp.sum(weights, axis=0, keepdims=True)
    weights = weights.astype(BF16)
    mixed_five = (dot(pairs[:, HEAD:], weights, ((0,), (0,))) / total).astype(BF16)
    partial = dot(mixed_five, decode_output, ((0,), (0,))).astype(BF16)
    arrived = exchange(partial.reshape(inner, rows, width), INNER)
    return last_sum(arrived, level_two)


def solution(mesh):
    outer, inner = mesh.shape["outer"], mesh.shape["inner"]
    finer = Mesh(mesh.devices.reshape(outer // 8, 4, 2, inner // 4, 4), AXES)
    placed = (
        P(ALL, None),
        P(OUTER, INNER),
        P(),
        P(),
        P(None, INNER),
        P(None, INNER),
        P(None, INNER),
        P(INNER, None),
        P(ALL, None),
        P(None, INNER),
        P(None, INNER),
        P(None, INNER),
        P(INNER, None),
    )
    return jax.shard_map(step, mesh=finer, in_specs=placed, out_specs=P(ALL, None), check_vma=False)
```

```python
import functools

import jax
import jax.numpy as jnp
from jax import lax
from jax.experimental import pallas as pl
from jax.experimental.pallas import tpu as pltpu
from jax.sharding import Mesh
from jax.sharding import PartitionSpec as P


HEAD = 128
AXES = ("y", "h", "c", "z", "x")
INNER = ("z", "x")
OUTER = ("y", "h", "c")
ALL = OUTER + INNER
BF16 = jnp.bfloat16
F32 = jnp.float32
SCALE = HEAD ** (-0.5)
TAIL = 16
PARAMS = pltpu.CompilerParams(vmem_limit_bytes=20 * 2**20)
WIDE = pltpu.CompilerParams(vmem_limit_bytes=62 * 2**20)


VMEM = pl.BlockSpec(memory_space=pltpu.VMEM)


def dot(a, b, dims):
    return lax.dot_general(a, b, (dims, ((), ())), preferred_element_type=F32)


def partner(value, axis, step):
    pairs = [(i, i ^ step) for i in range(lax.axis_size(axis))]
    return lax.ppermute(value, axis, pairs)


def exchange(tiles, axis):
    return lax.all_to_all(tiles, axis, split_axis=0, concat_axis=0, tiled=True)


def all_from(value, axis):
    copies = jnp.broadcast_to(value, (lax.axis_size(axis), *value.shape))
    return exchange(copies, axis)


def cost(flops, size):
    return pl.CostEstimate(flops=flops, bytes_accessed=size, transcendentals=0)


def key_kernel(slot_ref, group_ref, embed_ref, out_ref):
    lines = lax.broadcasted_iota(jnp.int32, embed_ref.shape, 0)
    chosen = jnp.where(lines == slot_ref[0, 0], embed_ref[...].astype(F32), 0.0)
    keyed = group_ref[...].astype(F32) + jnp.sum(chosen, axis=0, keepdims=True)
    block = keyed.astype(BF16)
    for j in range(out_ref.shape[0]):
        out_ref[j] = block


def key_copies(slot_ids, group_latents, slot_embed, many):
    return pl.pallas_call(
        key_kernel,
        out_shape=jax.ShapeDtypeStruct((many, *group_latents.shape), BF16),
        in_specs=[pl.BlockSpec(memory_space=pltpu.SMEM), VMEM, VMEM],
        out_specs=VMEM,
        compiler_params=WIDE,
        cost_estimate=cost(4 * group_latents.size, 2**20),
        name="key_copies",
    )(slot_ids, group_latents, slot_embed)


def attend_one(blocks_ref, pack):
    many = blocks_ref.shape[0]
    both = [dot(blocks_ref[j], pack, ((1,), (0,))) for j in range(many)]
    scores = jnp.concatenate([b[:, :-HEAD] for b in both], axis=0) * SCALE
    values = jnp.concatenate([b[:, -HEAD:].astype(BF16) for b in both], axis=0)
    top = jnp.max(scores, axis=0, keepdims=True)
    weights = jnp.exp(scores - top)
    total = jnp.sum(weights, axis=0, keepdims=True)
    mixed = dot(values, weights.astype(BF16), ((0,), (0,))) / total
    level = top + jnp.log(total)
    high = level.astype(BF16).astype(F32)
    middle = (level - high).astype(BF16).astype(F32)
    low = level - high - middle
    line = lax.broadcasted_iota(jnp.int32, (TAIL, mixed.shape[1]), 0)
    tail = jnp.where(line == 0, high, jnp.where(line == 1, middle, jnp.where(line == 2, low, 0.0)))
    return jnp.concatenate([mixed, tail], axis=0).astype(BF16)


def attend_kernel(blocks_ref, *refs):
    out_ref = refs[-1]
    mine = lax.axis_index("x")
    for k, pack_ref in enumerate(refs[:-1]):
        out_ref[mine ^ k] = attend_one(blocks_ref, pack_ref[...])


def attend_part(blocks, packs):
    many, length = len(packs), packs[0].shape[1] - HEAD
    keys = blocks.shape[0] * blocks.shape[1]
    flops = 2 * many * keys * (blocks.shape[2] * 2 * HEAD + HEAD * length)
    return pl.pallas_call(
        attend_kernel,
        out_shape=jax.ShapeDtypeStruct((many, HEAD + TAIL, length), BF16),
        in_specs=[VMEM] * (1 + many),
        out_specs=VMEM,
        compiler_params=WIDE,
        cost_estimate=cost(flops, 3 * 2**20),
        name="attend_part",
    )(blocks, *packs)


def pair_kernel(parts_ref, key_ref, value_ref, out_ref):
    lines = [parts_ref[j].astype(F32) for j in range(parts_ref.shape[0])]
    latents = jnp.concatenate(lines, axis=0).astype(BF16)
    out_ref[:, :HEAD] = dot(latents, key_ref[...], ((1,), (0,))).astype(BF16)
    out_ref[:, HEAD:] = dot(latents, value_ref[...], ((1,), (0,))).astype(BF16)


def decode_pairs(parts, key_weight, value_weight):
    rows = parts.shape[0] * parts.shape[1]
    return pl.pallas_call(
        pair_kernel,
        out_shape=jax.ShapeDtypeStruct((rows, 2 * HEAD), BF16),
        in_specs=[VMEM, VMEM, VMEM],
        out_specs=VMEM,
        compiler_params=PARAMS,
        cost_estimate=cost(4 * parts.size * HEAD, 2**20),
        name="decode_pairs",
    )(parts, key_weight, value_weight)


def join_kernel(parts_ref, weight_ref, out_ref):
    many = parts_ref.shape[0]
    levels = [
        jnp.sum(parts_ref[j, HEAD : HEAD + TAIL, :].astype(F32), axis=0, keepdims=True) for j in range(many)
    ]
    top = functools.reduce(jnp.maximum, levels)
    shares = [jnp.exp(level - top) for level in levels]
    total = functools.reduce(jnp.add, shares)
    mixed = functools.reduce(
        jnp.add, [parts_ref[j, :HEAD, :].astype(F32) * (shares[j] / total) for j in range(many)]
    )
    out_ref[...] = dot(mixed.astype(BF16), weight_ref[...], ((0,), (0,))).astype(BF16)


def join_and_project(parts, weight):
    length, width = parts.shape[2], weight.shape[1]
    return pl.pallas_call(
        join_kernel,
        out_shape=jax.ShapeDtypeStruct((length, width), BF16),
        in_specs=[VMEM, VMEM],
        out_specs=VMEM,
        compiler_params=PARAMS,
        cost_estimate=cost(2 * length * width * HEAD, 2**20),
        name="join_and_project",
    )(parts, weight)


def norm_kernel(parts_ref, own_ref, level_ref, copies_ref):
    many = parts_ref.shape[0]
    level = own_ref[...].astype(F32) + functools.reduce(
        jnp.add, [parts_ref[j].astype(F32) for j in range(many)]
    )
    level_ref[...] = level
    scale = lax.rsqrt(jnp.mean(level * level, axis=-1, keepdims=True) + 1e-06)
    normed = (level * scale).astype(BF16)
    for j in range(many):
        copies_ref[j] = normed


def sum_and_norm(parts, own):
    return pl.pallas_call(
        norm_kernel,
        out_shape=[
            jax.ShapeDtypeStruct(own.shape, F32),
            jax.ShapeDtypeStruct(parts.shape, BF16),
        ],
        in_specs=[VMEM, VMEM],
        out_specs=[VMEM, VMEM],
        compiler_params=PARAMS,
        cost_estimate=cost(4 * parts.size, 2**20),
        name="sum_and_norm",
    )(parts, own)


def last_kernel(parts_ref, level_ref, out_ref):
    total = functools.reduce(
        jnp.add, [parts_ref[j].astype(F32) for j in range(parts_ref.shape[0])]
    )
    out_ref[...] = (level_ref[...] + total).astype(BF16)


def last_sum(parts, level):
    return pl.pallas_call(
        last_kernel,
        out_shape=jax.ShapeDtypeStruct(level.shape, BF16),
        in_specs=[VMEM, VMEM],
        out_specs=VMEM,
        compiler_params=PARAMS,
        cost_estimate=cost(parts.size, 2**20),
        name="last_sum",
    )(parts, level)


def step(
    group_latents,
    slot_ids,
    slot_embed,
    merge_latents,
    query_weight,
    key_weight,
    value_weight,
    output_weight,
    global_latents,
    decode_query,
    decode_key,
    decode_value,
    decode_output,
):
    inner = lax.axis_size(INNER)
    length, width = merge_latents.shape
    rows = length // inner

    query_two = dot(merge_latents, query_weight, ((1,), (0,))).astype(BF16)
    folded = dot(key_weight, query_two, ((1,), (1,))).astype(BF16)
    pack = jnp.concatenate([folded, value_weight], axis=1)
    own_rows = lax.dynamic_slice_in_dim(merge_latents, lax.axis_index(INNER) * rows, rows, 0)

    copies = key_copies(slot_ids, group_latents, slot_embed, lax.axis_size("z"))
    blocks = exchange(copies, "z")
    pack_two = partner(pack, "x", 2)
    pack_three = partner(pack, "x", 3)
    pack_one = partner(pack, "x", 1)
    outer_block = all_from(global_latents, INNER)
    parts = attend_part(blocks, [pack, pack_one, pack_two, pack_three])
    parts = exchange(parts, "x")

    pairs = decode_pairs(outer_block, decode_key, decode_value)
    for axis, step_size in (("h", 1), ("h", 3), ("y", 1), ("y", 3)):
        if lax.axis_size(axis) > step_size:
            pairs = jnp.concatenate([pairs, partner(pairs, axis, step_size)], axis=0)
    other = partner(pairs, "c", 1)

    partial = join_and_project(parts, output_weight)
    arrived = exchange(partial.reshape(inner, rows, width), INNER)
    level_two, copies = sum_and_norm(arrived, own_rows)
    normed = exchange(copies, INNER).reshape(length, width)

    query_five = dot(normed, decode_query, ((1,), (0,))).astype(BF16)
    pairs = jnp.concatenate([pairs, other], axis=0)
    scores = dot(pairs[:, :HEAD], query_five, ((1,), (1,))) * SCALE
    top = jnp.max(scores, axis=0, keepdims=True)
    weights = jnp.exp(scores - top)
    total = jnp.sum(weights, axis=0, keepdims=True)
    weights = weights.astype(BF16)
    mixed_five = (dot(pairs[:, HEAD:], weights, ((0,), (0,))) / total).astype(BF16)
    partial = dot(mixed_five, decode_output, ((0,), (0,))).astype(BF16)
    arrived = exchange(partial.reshape(inner, rows, width), INNER)
    return last_sum(arrived, level_two)


def solution(mesh):
    outer, inner = mesh.shape["outer"], mesh.shape["inner"]
    finer = Mesh(mesh.devices.reshape(outer // 8, 4, 2, inner // 4, 4), AXES)
    placed = (
        P(ALL, None),
        P(OUTER, INNER),
        P(),
        P(),
        P(None, INNER),
        P(None, INNER),
        P(None, INNER),
        P(INNER, None),
        P(ALL, None),
        P(None, INNER),
        P(None, INNER),
        P(None, INNER),
        P(INNER, None),
    )
    return jax.shard_map(step, mesh=finer, in_specs=placed, out_specs=P(ALL, None), check_vma=False)
```

```python
import functools

import jax
import jax.numpy as jnp
from jax import lax
from jax.experimental import pallas as pl
from jax.experimental.pallas import tpu as pltpu
from jax.sharding import Mesh
from jax.sharding import PartitionSpec as P


HEAD = 128
AXES = ("y", "h", "c", "z", "x")
INNER = ("z", "x")
OUTER = ("y", "h", "c")
ALL = OUTER + INNER
BF16 = jnp.bfloat16
F32 = jnp.float32
SCALE = HEAD ** (-0.5)
TAIL = 16
PARAMS = pltpu.CompilerParams(vmem_limit_bytes=20 * 2**20)
WIDE = pltpu.CompilerParams(vmem_limit_bytes=62 * 2**20)


VMEM = pl.BlockSpec(memory_space=pltpu.VMEM)


def dot(a, b, dims):
    return lax.dot_general(a, b, (dims, ((), ())), preferred_element_type=F32)


def partner(value, axis, step):
    pairs = [(i, i ^ step) for i in range(lax.axis_size(axis))]
    return lax.ppermute(value, axis, pairs)


def exchange(tiles, axis):
    return lax.all_to_all(tiles, axis, split_axis=0, concat_axis=0, tiled=True)


def all_from(value, axis):
    copies = jnp.broadcast_to(value, (lax.axis_size(axis), *value.shape))
    return exchange(copies, axis)


def cost(flops, size):
    return pl.CostEstimate(flops=flops, bytes_accessed=size, transcendentals=0)


def key_kernel(slot_ref, group_ref, embed_ref, out_ref):
    lines = lax.broadcasted_iota(jnp.int32, embed_ref.shape, 0)
    chosen = jnp.where(lines == slot_ref[0, 0], embed_ref[...].astype(F32), 0.0)
    keyed = group_ref[...].astype(F32) + jnp.sum(chosen, axis=0, keepdims=True)
    out_ref[...] = keyed.astype(BF16)


def key_rows(slot_ids, group_latents, slot_embed):
    return pl.pallas_call(
        key_kernel,
        out_shape=jax.ShapeDtypeStruct(group_latents.shape, BF16),
        in_specs=[pl.BlockSpec(memory_space=pltpu.SMEM), VMEM, VMEM],
        out_specs=VMEM,
        compiler_params=WIDE,
        cost_estimate=cost(4 * group_latents.size, 2**20),
        name="key_rows",
    )(slot_ids, group_latents, slot_embed)


def attend_one(blocks_ref, pack):
    many = blocks_ref.shape[0]
    both = [dot(blocks_ref[j], pack, ((1,), (0,))) for j in range(many)]
    scores = jnp.concatenate([b[:, :-HEAD] for b in both], axis=0) * SCALE
    values = jnp.concatenate([b[:, -HEAD:].astype(BF16) for b in both], axis=0)
    top = jnp.max(scores, axis=0, keepdims=True)
    weights = jnp.exp(scores - top)
    total = jnp.sum(weights, axis=0, keepdims=True)
    mixed = dot(values, weights.astype(BF16), ((0,), (0,))) / total
    level = top + jnp.log(total)
    high = level.astype(BF16).astype(F32)
    middle = (level - high).astype(BF16).astype(F32)
    low = level - high - middle
    line = lax.broadcasted_iota(jnp.int32, (TAIL, mixed.shape[1]), 0)
    tail = jnp.where(line == 0, high, jnp.where(line == 1, middle, jnp.where(line == 2, low, 0.0)))
    return jnp.concatenate([mixed, tail], axis=0).astype(BF16)


def attend_kernel(count, *refs):
    given, (out_ref, blocks_ref, packs_ref, sems) = refs[:-4], refs[-4:]
    copies = []
    for k, ref in enumerate(given):
        target = blocks_ref.at[k] if k < count else packs_ref.at[k - count]
        copies.append(pltpu.make_async_copy(ref, target, sems.at[k]))
        copies[-1].start()
    for copy in copies[:count]:
        copy.wait()
    mine = lax.axis_index("x")
    for k, copy in enumerate(copies[count:]):
        copy.wait()
        out_ref[mine ^ k] = attend_one(blocks_ref, packs_ref[k])


def attend_part(blocks, packs):
    many, length = len(packs), packs[0].shape[1] - HEAD
    count = len(blocks)
    keys = count * blocks[0].shape[0]
    flops = 2 * many * keys * (blocks[0].shape[1] * 2 * HEAD + HEAD * length)
    return pl.pallas_call(
        functools.partial(attend_kernel, count),
        out_shape=jax.ShapeDtypeStruct((many, HEAD + TAIL, length), BF16),
        in_specs=[pl.BlockSpec(memory_space=pl.ANY)] * (count + many),
        out_specs=VMEM,
        scratch_shapes=[
            pltpu.VMEM((count, *blocks[0].shape), BF16),
            pltpu.VMEM((many, *packs[0].shape), BF16),
            pltpu.SemaphoreType.DMA((count + many,)),
        ],
        compiler_params=WIDE,
        cost_estimate=cost(flops, 3 * 2**20),
        name="attend_part",
    )(*blocks, *packs)


def pair_kernel(parts_ref, key_ref, value_ref, out_ref):
    lines = [parts_ref[j].astype(F32) for j in range(parts_ref.shape[0])]
    latents = jnp.concatenate(lines, axis=0).astype(BF16)
    out_ref[:, :HEAD] = dot(latents, key_ref[...], ((1,), (0,))).astype(BF16)
    out_ref[:, HEAD:] = dot(latents, value_ref[...], ((1,), (0,))).astype(BF16)


def decode_pairs(parts, key_weight, value_weight):
    rows = parts.shape[0] * parts.shape[1]
    return pl.pallas_call(
        pair_kernel,
        out_shape=jax.ShapeDtypeStruct((rows, 2 * HEAD), BF16),
        in_specs=[VMEM, VMEM, VMEM],
        out_specs=VMEM,
        compiler_params=PARAMS,
        cost_estimate=cost(4 * parts.size * HEAD, 2**20),
        name="decode_pairs",
    )(parts, key_weight, value_weight)


def join_kernel(parts_ref, weight_ref, out_ref):
    many = parts_ref.shape[0]
    levels = [
        jnp.sum(parts_ref[j, HEAD : HEAD + TAIL, :].astype(F32), axis=0, keepdims=True) for j in range(many)
    ]
    top = functools.reduce(jnp.maximum, levels)
    shares = [jnp.exp(level - top) for level in levels]
    total = functools.reduce(jnp.add, shares)
    mixed = functools.reduce(
        jnp.add, [parts_ref[j, :HEAD, :].astype(F32) * (shares[j] / total) for j in range(many)]
    )
    out_ref[...] = dot(mixed.astype(BF16), weight_ref[...], ((0,), (0,))).astype(BF16)


def join_and_project(parts, weight):
    length, width = parts.shape[2], weight.shape[1]
    return pl.pallas_call(
        join_kernel,
        out_shape=jax.ShapeDtypeStruct((length, width), BF16),
        in_specs=[VMEM, VMEM],
        out_specs=VMEM,
        compiler_params=PARAMS,
        cost_estimate=cost(2 * length * width * HEAD, 2**20),
        name="join_and_project",
    )(parts, weight)


def norm_kernel(parts_ref, own_ref, level_ref, copies_ref):
    many = parts_ref.shape[0]
    level = own_ref[...].astype(F32) + functools.reduce(
        jnp.add, [parts_ref[j].astype(F32) for j in range(many)]
    )
    level_ref[...] = level
    scale = lax.rsqrt(jnp.mean(level * level, axis=-1, keepdims=True) + 1e-06)
    normed = (level * scale).astype(BF16)
    for j in range(many):
        copies_ref[j] = normed


def sum_and_norm(parts, own):
    return pl.pallas_call(
        norm_kernel,
        out_shape=[
            jax.ShapeDtypeStruct(own.shape, F32),
            jax.ShapeDtypeStruct(parts.shape, BF16),
        ],
        in_specs=[VMEM, VMEM],
        out_specs=[VMEM, VMEM],
        compiler_params=PARAMS,
        cost_estimate=cost(4 * parts.size, 2**20),
        name="sum_and_norm",
    )(parts, own)


def last_kernel(parts_ref, level_ref, out_ref):
    total = functools.reduce(
        jnp.add, [parts_ref[j].astype(F32) for j in range(parts_ref.shape[0])]
    )
    out_ref[...] = (level_ref[...] + total).astype(BF16)


def last_sum(parts, level):
    return pl.pallas_call(
        last_kernel,
        out_shape=jax.ShapeDtypeStruct(level.shape, BF16),
        in_specs=[VMEM, VMEM],
        out_specs=VMEM,
        compiler_params=PARAMS,
        cost_estimate=cost(parts.size, 2**20),
        name="last_sum",
    )(parts, level)


def step(
    group_latents,
    slot_ids,
    slot_embed,
    merge_latents,
    query_weight,
    key_weight,
    value_weight,
    output_weight,
    global_latents,
    decode_query,
    decode_key,
    decode_value,
    decode_output,
):
    inner = lax.axis_size(INNER)
    length, width = merge_latents.shape
    rows = length // inner

    query_two = dot(merge_latents, query_weight, ((1,), (0,))).astype(BF16)
    folded = dot(key_weight, query_two, ((1,), (1,))).astype(BF16)
    pack = jnp.concatenate([folded, value_weight], axis=1)
    own_rows = lax.dynamic_slice_in_dim(merge_latents, lax.axis_index(INNER) * rows, rows, 0)

    keyed = key_rows(slot_ids, group_latents, slot_embed)
    pack_two = partner(pack, "x", 2)
    keyed_three = partner(keyed, "z", 3)
    outer_block = all_from(global_latents, INNER)
    pack_three = partner(pack, "x", 3)
    keyed_two = partner(keyed, "z", 2)
    pack_one = partner(pack, "x", 1)
    keyed_one = partner(keyed, "z", 1)
    parts = attend_part(
        [keyed, keyed_one, keyed_two, keyed_three],
        [pack, pack_one, pack_two, pack_three],
    )
    parts = exchange(parts, "x")

    pairs = decode_pairs(outer_block, decode_key, decode_value)
    for axis, step_size in (("h", 1), ("h", 3), ("y", 1), ("y", 3)):
        if lax.axis_size(axis) > step_size:
            pairs = jnp.concatenate([pairs, partner(pairs, axis, step_size)], axis=0)
    other = partner(pairs, "c", 1)

    partial = join_and_project(parts, output_weight)
    arrived = exchange(partial.reshape(inner, rows, width), INNER)
    level_two, copies = sum_and_norm(arrived, own_rows)
    normed = exchange(copies, INNER).reshape(length, width)

    query_five = dot(normed, decode_query, ((1,), (0,))).astype(BF16)
    pairs = jnp.concatenate([pairs, other], axis=0)
    scores = dot(pairs[:, :HEAD], query_five, ((1,), (1,))) * SCALE
    top = jnp.max(scores, axis=0, keepdims=True)
    weights = jnp.exp(scores - top)
    total = jnp.sum(weights, axis=0, keepdims=True)
    weights = weights.astype(BF16)
    mixed_five = (dot(pairs[:, HEAD:], weights, ((0,), (0,))) / total).astype(BF16)
    partial = dot(mixed_five, decode_output, ((0,), (0,))).astype(BF16)
    arrived = exchange(partial.reshape(inner, rows, width), INNER)
    return last_sum(arrived, level_two)


def solution(mesh):
    outer, inner = mesh.shape["outer"], mesh.shape["inner"]
    finer = Mesh(mesh.devices.reshape(outer // 8, 4, 2, inner // 4, 4), AXES)
    placed = (
        P(ALL, None),
        P(OUTER, INNER),
        P(),
        P(),
        P(None, INNER),
        P(None, INNER),
        P(None, INNER),
        P(INNER, None),
        P(ALL, None),
        P(None, INNER),
        P(None, INNER),
        P(None, INNER),
        P(INNER, None),
    )
    return jax.shard_map(step, mesh=finer, in_specs=placed, out_specs=P(ALL, None), check_vma=False)
```

```python
import functools

import jax
import jax.numpy as jnp
from jax import lax
from jax.experimental import pallas as pl
from jax.experimental.pallas import tpu as pltpu
from jax.sharding import Mesh
from jax.sharding import PartitionSpec as P


HEAD = 128
AXES = ("y", "h", "c", "z", "x")
INNER = ("z", "x")
OUTER = ("y", "h", "c")
ALL = OUTER + INNER
BF16 = jnp.bfloat16
F32 = jnp.float32
SCALE = HEAD ** (-0.5)
TAIL = 16
PARAMS = pltpu.CompilerParams(vmem_limit_bytes=20 * 2**20)
WIDE = pltpu.CompilerParams(vmem_limit_bytes=62 * 2**20)


VMEM = pl.BlockSpec(memory_space=pltpu.VMEM)


def dot(a, b, dims):
    return lax.dot_general(a, b, (dims, ((), ())), preferred_element_type=F32)


def partner(value, axis, step):
    pairs = [(i, i ^ step) for i in range(lax.axis_size(axis))]
    return lax.ppermute(value, axis, pairs)


def exchange(tiles, axis):
    return lax.all_to_all(tiles, axis, split_axis=0, concat_axis=0, tiled=True)


def all_from(value, axis):
    copies = jnp.broadcast_to(value, (lax.axis_size(axis), *value.shape))
    return exchange(copies, axis)


def cost(flops, size):
    return pl.CostEstimate(flops=flops, bytes_accessed=size, transcendentals=0)


def prepare_kernel(
    slot_ref, group_ref, embed_ref, merge_ref, query_ref, key_ref, value_ref, keyed_ref, pack_ref
):
    lines = lax.broadcasted_iota(jnp.int32, embed_ref.shape, 0)
    chosen = jnp.where(lines == slot_ref[0, 0], embed_ref[...].astype(F32), 0.0)
    keyed = group_ref[...].astype(F32) + jnp.sum(chosen, axis=0, keepdims=True)
    keyed_ref[...] = keyed.astype(BF16)
    query = dot(merge_ref[...], query_ref[...], ((1,), (0,))).astype(BF16)
    length = query.shape[0]
    pack_ref[:, :length] = dot(key_ref[...], query, ((1,), (1,))).astype(BF16)
    pack_ref[:, length:] = value_ref[...]


def prepare(slot_ids, group_latents, slot_embed, merge_latents, query, key, value):
    depth, columns = key.shape
    return pl.pallas_call(
        prepare_kernel,
        out_shape=[
            jax.ShapeDtypeStruct(group_latents.shape, BF16),
            jax.ShapeDtypeStruct((depth, merge_latents.shape[0] + columns), BF16),
        ],
        in_specs=[pl.BlockSpec(memory_space=pltpu.SMEM)] + [VMEM] * 6,
        out_specs=[VMEM, VMEM],
        compiler_params=WIDE,
        cost_estimate=cost(2 * merge_latents.size * columns * 2, 2**20),
        name="prepare",
    )(slot_ids, group_latents, slot_embed, merge_latents, query, key, value)


def attend_one(blocks, pack):
    both = dot(blocks, pack, ((1,), (0,)))
    scores = both[:, :-HEAD] * SCALE
    values = both[:, -HEAD:].astype(BF16)
    top = jnp.max(scores, axis=0, keepdims=True)
    weights = jnp.exp(scores - top)
    total = jnp.sum(weights, axis=0, keepdims=True)
    mixed = dot(values, weights.astype(BF16), ((0,), (0,))) / total
    level = top + jnp.log(total)
    high = level.astype(BF16).astype(F32)
    middle = (level - high).astype(BF16).astype(F32)
    low = level - high - middle
    line = lax.broadcasted_iota(jnp.int32, (TAIL, mixed.shape[1]), 0)
    tail = jnp.where(line == 0, high, jnp.where(line == 1, middle, jnp.where(line == 2, low, 0.0)))
    return jnp.concatenate([mixed, tail], axis=0).astype(BF16)


def attend_kernel(count, *refs):
    given, (out_ref, blocks_ref, packs_ref, sems) = refs[:-4], refs[-4:]
    size = given[0].shape[0]
    copies = []
    for k, ref in enumerate(given):
        target = blocks_ref.at[pl.ds(k * size, size)] if k < count else packs_ref.at[k - count]
        copies.append(pltpu.make_async_copy(ref, target, sems.at[k]))
        copies[-1].start()
    for copy in copies[:count]:
        copy.wait()
    mine = lax.axis_index("x")
    for k, copy in enumerate(copies[count:]):
        copy.wait()
        out_ref[mine ^ k] = attend_one(blocks_ref[...], packs_ref[k])


def attend_part(blocks, packs):
    many, length = len(packs), packs[0].shape[1] - HEAD
    count = len(blocks)
    keys = count * blocks[0].shape[0]
    flops = 2 * many * keys * (blocks[0].shape[1] * 2 * HEAD + HEAD * length)
    return pl.pallas_call(
        functools.partial(attend_kernel, count),
        out_shape=jax.ShapeDtypeStruct((many, HEAD + TAIL, length), BF16),
        in_specs=[pl.BlockSpec(memory_space=pl.ANY)] * (count + many),
        out_specs=VMEM,
        scratch_shapes=[
            pltpu.VMEM((keys, blocks[0].shape[1]), BF16),
            pltpu.VMEM((many, *packs[0].shape), BF16),
            pltpu.SemaphoreType.DMA((count + many,)),
        ],
        compiler_params=WIDE,
        cost_estimate=cost(flops, 3 * 2**20),
        name="attend_part",
    )(*blocks, *packs)


def pair_kernel(parts_ref, key_ref, value_ref, out_ref):
    lines = [parts_ref[j].astype(F32) for j in range(parts_ref.shape[0])]
    latents = jnp.concatenate(lines, axis=0).astype(BF16)
    out_ref[:, :HEAD] = dot(latents, key_ref[...], ((1,), (0,))).astype(BF16)
    out_ref[:, HEAD:] = dot(latents, value_ref[...], ((1,), (0,))).astype(BF16)


def decode_pairs(parts, key_weight, value_weight):
    rows = parts.shape[0] * parts.shape[1]
    return pl.pallas_call(
        pair_kernel,
        out_shape=jax.ShapeDtypeStruct((rows, 2 * HEAD), BF16),
        in_specs=[VMEM, VMEM, VMEM],
        out_specs=VMEM,
        compiler_params=PARAMS,
        cost_estimate=cost(4 * parts.size * HEAD, 2**20),
        name="decode_pairs",
    )(parts, key_weight, value_weight)


def join_kernel(parts_ref, weight_ref, out_ref):
    many = parts_ref.shape[0]
    levels = [
        jnp.sum(parts_ref[j, HEAD : HEAD + TAIL, :].astype(F32), axis=0, keepdims=True) for j in range(many)
    ]
    top = functools.reduce(jnp.maximum, levels)
    shares = [jnp.exp(level - top) for level in levels]
    total = functools.reduce(jnp.add, shares)
    mixed = functools.reduce(
        jnp.add, [parts_ref[j, :HEAD, :].astype(F32) * (shares[j] / total) for j in range(many)]
    )
    out_ref[...] = dot(mixed.astype(BF16), weight_ref[...], ((0,), (0,))).astype(BF16)


def join_and_project(parts, weight):
    length, width = parts.shape[2], weight.shape[1]
    return pl.pallas_call(
        join_kernel,
        out_shape=jax.ShapeDtypeStruct((length, width), BF16),
        in_specs=[VMEM, VMEM],
        out_specs=VMEM,
        compiler_params=PARAMS,
        cost_estimate=cost(2 * length * width * HEAD, 2**20),
        name="join_and_project",
    )(parts, weight)


def norm_kernel(parts_ref, own_ref, level_ref, copies_ref):
    many = parts_ref.shape[0]
    level = own_ref[...].astype(F32) + functools.reduce(
        jnp.add, [parts_ref[j].astype(F32) for j in range(many)]
    )
    level_ref[...] = level
    scale = lax.rsqrt(jnp.mean(level * level, axis=-1, keepdims=True) + 1e-06)
    normed = (level * scale).astype(BF16)
    for j in range(many):
        copies_ref[j] = normed


def sum_and_norm(parts, own):
    return pl.pallas_call(
        norm_kernel,
        out_shape=[
            jax.ShapeDtypeStruct(own.shape, F32),
            jax.ShapeDtypeStruct(parts.shape, BF16),
        ],
        in_specs=[VMEM, VMEM],
        out_specs=[VMEM, VMEM],
        compiler_params=PARAMS,
        cost_estimate=cost(4 * parts.size, 2**20),
        name="sum_and_norm",
    )(parts, own)


def last_kernel(parts_ref, level_ref, out_ref):
    total = functools.reduce(
        jnp.add, [parts_ref[j].astype(F32) for j in range(parts_ref.shape[0])]
    )
    out_ref[...] = (level_ref[...] + total).astype(BF16)


def last_sum(parts, level):
    return pl.pallas_call(
        last_kernel,
        out_shape=jax.ShapeDtypeStruct(level.shape, BF16),
        in_specs=[VMEM, VMEM],
        out_specs=VMEM,
        compiler_params=PARAMS,
        cost_estimate=cost(parts.size, 2**20),
        name="last_sum",
    )(parts, level)


def step(
    group_latents,
    slot_ids,
    slot_embed,
    merge_latents,
    query_weight,
    key_weight,
    value_weight,
    output_weight,
    global_latents,
    decode_query,
    decode_key,
    decode_value,
    decode_output,
):
    inner = lax.axis_size(INNER)
    length, width = merge_latents.shape
    rows = length // inner

    own_rows = lax.dynamic_slice_in_dim(merge_latents, lax.axis_index(INNER) * rows, rows, 0)

    keyed, pack = prepare(
        slot_ids, group_latents, slot_embed, merge_latents, query_weight, key_weight, value_weight
    )
    pack_two = partner(pack, "x", 2)
    keyed_three = partner(keyed, "z", 3)
    outer_block = all_from(global_latents, INNER)
    pack_three = partner(pack, "x", 3)
    keyed_two = partner(keyed, "z", 2)
    pack_one = partner(pack, "x", 1)
    keyed_one = partner(keyed, "z", 1)
    parts = attend_part(
        [keyed, keyed_one, keyed_two, keyed_three],
        [pack, pack_one, pack_two, pack_three],
    )
    parts = exchange(parts, "x")

    pairs = decode_pairs(outer_block, decode_key, decode_value)
    for axis, step_size in (("h", 1), ("h", 3), ("y", 1), ("y", 3)):
        if lax.axis_size(axis) > step_size:
            pairs = jnp.concatenate([pairs, partner(pairs, axis, step_size)], axis=0)
    other = partner(pairs, "c", 1)

    partial = join_and_project(parts, output_weight)
    arrived = exchange(partial.reshape(inner, rows, width), INNER)
    level_two, copies = sum_and_norm(arrived, own_rows)
    normed = exchange(copies, INNER).reshape(length, width)

    query_five = dot(normed, decode_query, ((1,), (0,))).astype(BF16)
    pairs = jnp.concatenate([pairs, other], axis=0)
    scores = dot(pairs[:, :HEAD], query_five, ((1,), (1,))) * SCALE
    top = jnp.max(scores, axis=0, keepdims=True)
    weights = jnp.exp(scores - top)
    total = jnp.sum(weights, axis=0, keepdims=True)
    weights = weights.astype(BF16)
    mixed_five = (dot(pairs[:, HEAD:], weights, ((0,), (0,))) / total).astype(BF16)
    partial = dot(mixed_five, decode_output, ((0,), (0,))).astype(BF16)
    arrived = exchange(partial.reshape(inner, rows, width), INNER)
    return last_sum(arrived, level_two)


def solution(mesh):
    outer, inner = mesh.shape["outer"], mesh.shape["inner"]
    finer = Mesh(mesh.devices.reshape(outer // 8, 4, 2, inner // 4, 4), AXES)
    placed = (
        P(ALL, None),
        P(OUTER, INNER),
        P(),
        P(),
        P(None, INNER),
        P(None, INNER),
        P(None, INNER),
        P(INNER, None),
        P(ALL, None),
        P(None, INNER),
        P(None, INNER),
        P(None, INNER),
        P(INNER, None),
    )
    return jax.shard_map(step, mesh=finer, in_specs=placed, out_specs=P(ALL, None), check_vma=False)
```

```python
import functools

import jax
import jax.numpy as jnp
from jax import lax
from jax.experimental import pallas as pl
from jax.experimental.pallas import tpu as pltpu
from jax.sharding import Mesh
from jax.sharding import PartitionSpec as P


HEAD = 128
AXES = ("y", "h", "c", "z", "x")
INNER = ("z", "x")
OUTER = ("y", "h", "c")
ALL = OUTER + INNER
BF16 = jnp.bfloat16
F32 = jnp.float32
SCALE = HEAD ** (-0.5)
TAIL = 16
PARAMS = pltpu.CompilerParams(vmem_limit_bytes=20 * 2**20)
WIDE = pltpu.CompilerParams(vmem_limit_bytes=62 * 2**20)


VMEM = pl.BlockSpec(memory_space=pltpu.VMEM)


def dot(a, b, dims):
    return lax.dot_general(a, b, (dims, ((), ())), preferred_element_type=F32)


def partner(value, axis, step):
    pairs = [(i, i ^ step) for i in range(lax.axis_size(axis))]
    return lax.ppermute(value, axis, pairs)


def exchange(tiles, axis):
    return lax.all_to_all(tiles, axis, split_axis=0, concat_axis=0, tiled=True)


def all_from(value, axis):
    copies = jnp.broadcast_to(value, (lax.axis_size(axis), *value.shape))
    return exchange(copies, axis)


def cost(flops, size):
    return pl.CostEstimate(flops=flops, bytes_accessed=size, transcendentals=0)


def prepare_kernel(
    slot_ref, group_ref, embed_ref, merge_ref, query_ref, key_ref, value_ref, keyed_ref, pack_ref
):
    lines = lax.broadcasted_iota(jnp.int32, embed_ref.shape, 0)
    chosen = jnp.where(lines == slot_ref[0, 0], embed_ref[...].astype(F32), 0.0)
    keyed = group_ref[...].astype(F32) + jnp.sum(chosen, axis=0, keepdims=True)
    keyed_ref[...] = keyed.astype(BF16)
    query = dot(merge_ref[...], query_ref[...], ((1,), (0,))).astype(BF16)
    length = query.shape[0]
    pack_ref[:, :length] = dot(key_ref[...], query, ((1,), (1,))).astype(BF16)
    pack_ref[:, length:] = value_ref[...]


def prepare(slot_ids, group_latents, slot_embed, merge_latents, query, key, value):
    depth, columns = key.shape
    return pl.pallas_call(
        prepare_kernel,
        out_shape=[
            jax.ShapeDtypeStruct(group_latents.shape, BF16),
            jax.ShapeDtypeStruct((depth, merge_latents.shape[0] + columns), BF16),
        ],
        in_specs=[pl.BlockSpec(memory_space=pltpu.SMEM)] + [VMEM] * 6,
        out_specs=[VMEM, VMEM],
        compiler_params=WIDE,
        cost_estimate=cost(2 * merge_latents.size * columns * 2, 2**20),
        name="prepare",
    )(slot_ids, group_latents, slot_embed, merge_latents, query, key, value)


def attend_blocks(blocks, pack):
    both = [dot(block[...], pack, ((1,), (0,))) for block in blocks]
    scores = jnp.concatenate([b[:, :-HEAD] for b in both], axis=0) * SCALE
    values = jnp.concatenate([b[:, -HEAD:].astype(BF16) for b in both], axis=0)
    return scores, values


def early_kernel(count, *refs):
    blocks, packs, (mixed_ref, state_ref) = refs[:count], refs[count:-2], refs[-2:]
    for k, pack_ref in enumerate(packs):
        scores, values = attend_blocks(blocks, pack_ref[...])
        top = jnp.max(scores, axis=0, keepdims=True)
        weights = jnp.exp(scores - top)
        state_ref[k, :8, :] = jnp.broadcast_to(top, (8, top.shape[1]))
        state_ref[k, 8:, :] = jnp.broadcast_to(
            jnp.sum(weights, axis=0, keepdims=True), (8, top.shape[1])
        )
        mixed_ref[k] = dot(values, weights.astype(BF16), ((0,), (0,)))


def late_kernel(count, *refs):
    blocks, packs = refs[:count], refs[count:-3]
    mixed_ref, state_ref, out_ref = refs[-3:]
    mine = lax.axis_index("x")
    for k, pack_ref in enumerate(packs):
        scores, values = attend_blocks(blocks, pack_ref[...])
        before = state_ref[k, :1, :]
        top = jnp.maximum(jnp.max(scores, axis=0, keepdims=True), before)
        weights = jnp.exp(scores - top)
        kept = jnp.exp(before - top)
        total = jnp.sum(weights, axis=0, keepdims=True) + state_ref[k, 8:9, :] * kept
        mixed = dot(values, weights.astype(BF16), ((0,), (0,))) + mixed_ref[k] * kept
        mixed = mixed / total
        level = top + jnp.log(total)
        high = level.astype(BF16).astype(F32)
        middle = (level - high).astype(BF16).astype(F32)
        low = level - high - middle
        line = lax.broadcasted_iota(jnp.int32, (TAIL, mixed.shape[1]), 0)
        tail = jnp.where(
            line == 0, high, jnp.where(line == 1, middle, jnp.where(line == 2, low, 0.0))
        )
        out_ref[mine ^ k] = jnp.concatenate([mixed, tail], axis=0).astype(BF16)


def attend_cost(blocks, packs):
    keys = len(blocks) * blocks[0].shape[0]
    flops = 2 * len(packs) * keys * packs[0].size + 2 * len(packs) * keys * HEAD * HEAD
    return cost(flops, 3 * 2**20)


def attend_early(blocks, packs):
    many, length = len(packs), packs[0].shape[1] - HEAD
    return pl.pallas_call(
        functools.partial(early_kernel, len(blocks)),
        out_shape=[
            jax.ShapeDtypeStruct((many, HEAD, length), F32),
            jax.ShapeDtypeStruct((many, 16, length), F32),
        ],
        in_specs=[VMEM] * (len(blocks) + many),
        out_specs=[VMEM, VMEM],
        compiler_params=WIDE,
        cost_estimate=attend_cost(blocks, packs),
        name="attend_early",
    )(*blocks, *packs)


def attend_late(blocks, packs, mixed, state):
    many, length = len(packs), packs[0].shape[1] - HEAD
    return pl.pallas_call(
        functools.partial(late_kernel, len(blocks)),
        out_shape=jax.ShapeDtypeStruct((many, HEAD + TAIL, length), BF16),
        in_specs=[VMEM] * (len(blocks) + many + 2),
        out_specs=VMEM,
        compiler_params=WIDE,
        cost_estimate=attend_cost(blocks, packs),
        name="attend_late",
    )(*blocks, *packs, mixed, state)


def pair_kernel(parts_ref, key_ref, value_ref, out_ref):
    lines = [parts_ref[j].astype(F32) for j in range(parts_ref.shape[0])]
    latents = jnp.concatenate(lines, axis=0).astype(BF16)
    out_ref[:, :HEAD] = dot(latents, key_ref[...], ((1,), (0,))).astype(BF16)
    out_ref[:, HEAD:] = dot(latents, value_ref[...], ((1,), (0,))).astype(BF16)


def decode_pairs(parts, key_weight, value_weight):
    rows = parts.shape[0] * parts.shape[1]
    return pl.pallas_call(
        pair_kernel,
        out_shape=jax.ShapeDtypeStruct((rows, 2 * HEAD), BF16),
        in_specs=[VMEM, VMEM, VMEM],
        out_specs=VMEM,
        compiler_params=PARAMS,
        cost_estimate=cost(4 * parts.size * HEAD, 2**20),
        name="decode_pairs",
    )(parts, key_weight, value_weight)


def join_kernel(parts_ref, weight_ref, out_ref):
    many = parts_ref.shape[0]
    levels = [
        jnp.sum(parts_ref[j, HEAD : HEAD + TAIL, :].astype(F32), axis=0, keepdims=True) for j in range(many)
    ]
    top = functools.reduce(jnp.maximum, levels)
    shares = [jnp.exp(level - top) for level in levels]
    total = functools.reduce(jnp.add, shares)
    mixed = functools.reduce(
        jnp.add, [parts_ref[j, :HEAD, :].astype(F32) * (shares[j] / total) for j in range(many)]
    )
    out_ref[...] = dot(mixed.astype(BF16), weight_ref[...], ((0,), (0,))).astype(BF16)


def join_and_project(parts, weight):
    length, width = parts.shape[2], weight.shape[1]
    return pl.pallas_call(
        join_kernel,
        out_shape=jax.ShapeDtypeStruct((length, width), BF16),
        in_specs=[VMEM, VMEM],
        out_specs=VMEM,
        compiler_params=PARAMS,
        cost_estimate=cost(2 * length * width * HEAD, 2**20),
        name="join_and_project",
    )(parts, weight)


def norm_kernel(parts_ref, own_ref, level_ref, copies_ref):
    many = parts_ref.shape[0]
    level = own_ref[...].astype(F32) + functools.reduce(
        jnp.add, [parts_ref[j].astype(F32) for j in range(many)]
    )
    level_ref[...] = level
    scale = lax.rsqrt(jnp.mean(level * level, axis=-1, keepdims=True) + 1e-06)
    normed = (level * scale).astype(BF16)
    for j in range(many):
        copies_ref[j] = normed


def sum_and_norm(parts, own):
    return pl.pallas_call(
        norm_kernel,
        out_shape=[
            jax.ShapeDtypeStruct(own.shape, F32),
            jax.ShapeDtypeStruct(parts.shape, BF16),
        ],
        in_specs=[VMEM, VMEM],
        out_specs=[VMEM, VMEM],
        compiler_params=PARAMS,
        cost_estimate=cost(4 * parts.size, 2**20),
        name="sum_and_norm",
    )(parts, own)


def last_kernel(parts_ref, level_ref, out_ref):
    total = functools.reduce(
        jnp.add, [parts_ref[j].astype(F32) for j in range(parts_ref.shape[0])]
    )
    out_ref[...] = (level_ref[...] + total).astype(BF16)


def last_sum(parts, level):
    return pl.pallas_call(
        last_kernel,
        out_shape=jax.ShapeDtypeStruct(level.shape, BF16),
        in_specs=[VMEM, VMEM],
        out_specs=VMEM,
        compiler_params=PARAMS,
        cost_estimate=cost(parts.size, 2**20),
        name="last_sum",
    )(parts, level)


def step(
    group_latents,
    slot_ids,
    slot_embed,
    merge_latents,
    query_weight,
    key_weight,
    value_weight,
    output_weight,
    global_latents,
    decode_query,
    decode_key,
    decode_value,
    decode_output,
):
    inner = lax.axis_size(INNER)
    length, width = merge_latents.shape
    rows = length // inner

    own_rows = lax.dynamic_slice_in_dim(merge_latents, lax.axis_index(INNER) * rows, rows, 0)

    keyed, pack = prepare(
        slot_ids, group_latents, slot_embed, merge_latents, query_weight, key_weight, value_weight
    )
    pack_two = partner(pack, "x", 2)
    keyed_three = partner(keyed, "z", 3)
    outer_block = all_from(global_latents, ("c", *INNER))
    pack_three = partner(pack, "x", 3)
    keyed_two = partner(keyed, "z", 2)
    pack_one = partner(pack, "x", 1)
    keyed_one = partner(keyed, "z", 1)
    packs = [pack, pack_one, pack_two, pack_three]
    mixed, state = attend_early([keyed, keyed_three], packs)
    parts = attend_late([keyed_two, keyed_one], packs, mixed, state)
    parts = exchange(parts, "x")

    pairs = decode_pairs(outer_block, decode_key, decode_value)
    for axis, step_size in (("h", 1), ("h", 3), ("y", 1), ("y", 3)):
        if lax.axis_size(axis) > step_size:
            pairs = jnp.concatenate([pairs, partner(pairs, axis, step_size)], axis=0)

    partial = join_and_project(parts, output_weight)
    arrived = exchange(partial.reshape(inner, rows, width), INNER)
    level_two, copies = sum_and_norm(arrived, own_rows)
    normed = exchange(copies, INNER).reshape(length, width)

    query_five = dot(normed, decode_query, ((1,), (0,))).astype(BF16)
    scores = dot(pairs[:, :HEAD], query_five, ((1,), (1,))) * SCALE
    top = jnp.max(scores, axis=0, keepdims=True)
    weights = jnp.exp(scores - top)
    total = jnp.sum(weights, axis=0, keepdims=True)
    weights = weights.astype(BF16)
    mixed_five = (dot(pairs[:, HEAD:], weights, ((0,), (0,))) / total).astype(BF16)
    partial = dot(mixed_five, decode_output, ((0,), (0,))).astype(BF16)
    arrived = exchange(partial.reshape(inner, rows, width), INNER)
    return last_sum(arrived, level_two)


def solution(mesh):
    outer, inner = mesh.shape["outer"], mesh.shape["inner"]
    finer = Mesh(mesh.devices.reshape(outer // 8, 4, 2, inner // 4, 4), AXES)
    placed = (
        P(ALL, None),
        P(OUTER, INNER),
        P(),
        P(),
        P(None, INNER),
        P(None, INNER),
        P(None, INNER),
        P(INNER, None),
        P(ALL, None),
        P(None, INNER),
        P(None, INNER),
        P(None, INNER),
        P(INNER, None),
    )
    return jax.shard_map(step, mesh=finer, in_specs=placed, out_specs=P(ALL, None), check_vma=False)
```

```python
import functools

import jax
import jax.numpy as jnp
from jax import lax
from jax.experimental import pallas as pl
from jax.experimental.pallas import tpu as pltpu
from jax.sharding import Mesh
from jax.sharding import PartitionSpec as P


HEAD = 128
AXES = ("y", "h", "c", "z", "x")
INNER = ("z", "x")
OUTER = ("y", "h", "c")
ALL = OUTER + INNER
BF16 = jnp.bfloat16
F32 = jnp.float32
SCALE = HEAD ** (-0.5)
TAIL = 16
ROWS = 256
PARAMS = pltpu.CompilerParams(vmem_limit_bytes=20 * 2**20)
WIDE = pltpu.CompilerParams(vmem_limit_bytes=62 * 2**20)


VMEM = pl.BlockSpec(memory_space=pltpu.VMEM)


def dot(a, b, dims):
    return lax.dot_general(a, b, (dims, ((), ())), preferred_element_type=F32)


def partner(value, axis, step):
    pairs = [(i, i ^ step) for i in range(lax.axis_size(axis))]
    return lax.ppermute(value, axis, pairs)


def exchange(tiles, axis):
    return lax.all_to_all(tiles, axis, split_axis=0, concat_axis=0, tiled=True)


def all_from(value, axis):
    copies = jnp.broadcast_to(value, (lax.axis_size(axis), *value.shape))
    return exchange(copies, axis)


def cost(flops, size):
    return pl.CostEstimate(flops=flops, bytes_accessed=size, transcendentals=0)


def prepare_kernel(
    slot_ref, group_ref, embed_ref, merge_ref, query_ref, key_ref, value_ref, keyed_ref, pack_ref
):
    lines = lax.broadcasted_iota(jnp.int32, embed_ref.shape, 0)
    chosen = jnp.where(lines == slot_ref[0, 0], embed_ref[...].astype(F32), 0.0)
    keyed = group_ref[...].astype(F32) + jnp.sum(chosen, axis=0, keepdims=True)
    keyed_ref[...] = keyed.astype(BF16)
    query = dot(merge_ref[...], query_ref[...], ((1,), (0,))).astype(BF16)
    length = query.shape[0]
    pack_ref[:, :length] = dot(key_ref[...], query, ((1,), (1,))).astype(BF16)
    pack_ref[:, length:] = value_ref[...]


def prepare(slot_ids, group_latents, slot_embed, merge_latents, query, key, value):
    depth, columns = key.shape
    return pl.pallas_call(
        prepare_kernel,
        out_shape=[
            jax.ShapeDtypeStruct(group_latents.shape, BF16),
            jax.ShapeDtypeStruct((depth, merge_latents.shape[0] + columns), BF16),
        ],
        in_specs=[pl.BlockSpec(memory_space=pltpu.SMEM)] + [VMEM] * 6,
        out_specs=[VMEM, VMEM],
        compiler_params=WIDE,
        cost_estimate=cost(2 * merge_latents.size * columns * 2, 2**20),
        name="prepare",
    )(slot_ids, group_latents, slot_embed, merge_latents, query, key, value)


def attend_one(blocks_ref, pack):
    both = [
        dot(blocks_ref[pl.ds(k, ROWS)], pack, ((1,), (0,)))
        for k in range(0, blocks_ref.shape[0], ROWS)
    ]
    scores = jnp.concatenate([b[:, :-HEAD] for b in both], axis=0) * SCALE
    values = jnp.concatenate([b[:, -HEAD:].astype(BF16) for b in both], axis=0)
    top = jnp.max(scores, axis=0, keepdims=True)
    weights = jnp.exp(scores - top)
    total = jnp.sum(weights, axis=0, keepdims=True)
    mixed = dot(values, weights.astype(BF16), ((0,), (0,))) / total
    level = top + jnp.log(total)
    high = level.astype(BF16).astype(F32)
    middle = (level - high).astype(BF16).astype(F32)
    low = level - high - middle
    line = lax.broadcasted_iota(jnp.int32, (TAIL, mixed.shape[1]), 0)
    tail = jnp.where(line == 0, high, jnp.where(line == 1, middle, jnp.where(line == 2, low, 0.0)))
    return jnp.concatenate([mixed, tail], axis=0).astype(BF16)


def attend_kernel(count, *refs):
    given, (out_ref, blocks_ref, packs_ref, sems) = refs[:-4], refs[-4:]
    size = given[0].shape[0]
    copies = []
    for k, ref in enumerate(given):
        target = blocks_ref.at[pl.ds(k * size, size)] if k < count else packs_ref.at[k - count]
        copies.append(pltpu.make_async_copy(ref, target, sems.at[k]))
        copies[-1].start()
    for copy in copies[:count]:
        copy.wait()
    mine = lax.axis_index("x")
    for k, copy in enumerate(copies[count:]):
        copy.wait()
        out_ref[mine ^ k] = attend_one(blocks_ref, packs_ref[k])


def attend_part(blocks, packs):
    many, length = len(packs), packs[0].shape[1] - HEAD
    count = len(blocks)
    keys = count * blocks[0].shape[0]
    flops = 2 * many * keys * (blocks[0].shape[1] * 2 * HEAD + HEAD * length)
    return pl.pallas_call(
        functools.partial(attend_kernel, count),
        out_shape=jax.ShapeDtypeStruct((many, HEAD + TAIL, length), BF16),
        in_specs=[pl.BlockSpec(memory_space=pl.ANY)] * (count + many),
        out_specs=VMEM,
        scratch_shapes=[
            pltpu.VMEM((keys, blocks[0].shape[1]), BF16),
            pltpu.VMEM((many, *packs[0].shape), BF16),
            pltpu.SemaphoreType.DMA((count + many,)),
        ],
        compiler_params=PARAMS,
        cost_estimate=cost(flops, 3 * 2**20),
        name="attend_part",
    )(*blocks, *packs)


def pair_kernel(parts_ref, key_ref, value_ref, out_ref):
    lines = [parts_ref[j].astype(F32) for j in range(parts_ref.shape[0])]
    latents = jnp.concatenate(lines, axis=0).astype(BF16)
    out_ref[:, :HEAD] = dot(latents, key_ref[...], ((1,), (0,))).astype(BF16)
    out_ref[:, HEAD:] = dot(latents, value_ref[...], ((1,), (0,))).astype(BF16)


def decode_pairs(parts, key_weight, value_weight):
    rows = parts.shape[0] * parts.shape[1]
    return pl.pallas_call(
        pair_kernel,
        out_shape=jax.ShapeDtypeStruct((rows, 2 * HEAD), BF16),
        in_specs=[VMEM, VMEM, VMEM],
        out_specs=VMEM,
        compiler_params=PARAMS,
        cost_estimate=cost(4 * parts.size * HEAD, 2**20),
        name="decode_pairs",
    )(parts, key_weight, value_weight)


def join_kernel(parts_ref, weight_ref, out_ref):
    many = parts_ref.shape[0]
    levels = [
        jnp.sum(parts_ref[j, HEAD : HEAD + TAIL, :].astype(F32), axis=0, keepdims=True) for j in range(many)
    ]
    top = functools.reduce(jnp.maximum, levels)
    shares = [jnp.exp(level - top) for level in levels]
    total = functools.reduce(jnp.add, shares)
    mixed = functools.reduce(
        jnp.add, [parts_ref[j, :HEAD, :].astype(F32) * (shares[j] / total) for j in range(many)]
    )
    out_ref[...] = dot(mixed.astype(BF16), weight_ref[...], ((0,), (0,))).astype(BF16)


def join_and_project(parts, weight):
    length, width = parts.shape[2], weight.shape[1]
    return pl.pallas_call(
        join_kernel,
        out_shape=jax.ShapeDtypeStruct((length, width), BF16),
        in_specs=[VMEM, VMEM],
        out_specs=VMEM,
        compiler_params=PARAMS,
        cost_estimate=cost(2 * length * width * HEAD, 2**20),
        name="join_and_project",
    )(parts, weight)


def norm_kernel(parts_ref, own_ref, level_ref, copies_ref):
    many = parts_ref.shape[0]
    level = own_ref[...].astype(F32) + functools.reduce(
        jnp.add, [parts_ref[j].astype(F32) for j in range(many)]
    )
    level_ref[...] = level
    scale = lax.rsqrt(jnp.mean(level * level, axis=-1, keepdims=True) + 1e-06)
    normed = (level * scale).astype(BF16)
    for j in range(many):
        copies_ref[j] = normed


def sum_and_norm(parts, own):
    return pl.pallas_call(
        norm_kernel,
        out_shape=[
            jax.ShapeDtypeStruct(own.shape, F32),
            jax.ShapeDtypeStruct(parts.shape, BF16),
        ],
        in_specs=[VMEM, VMEM],
        out_specs=[VMEM, VMEM],
        compiler_params=PARAMS,
        cost_estimate=cost(4 * parts.size, 2**20),
        name="sum_and_norm",
    )(parts, own)


def last_kernel(parts_ref, level_ref, out_ref):
    total = functools.reduce(
        jnp.add, [parts_ref[j].astype(F32) for j in range(parts_ref.shape[0])]
    )
    out_ref[...] = (level_ref[...] + total).astype(BF16)


def last_sum(parts, level):
    return pl.pallas_call(
        last_kernel,
        out_shape=jax.ShapeDtypeStruct(level.shape, BF16),
        in_specs=[VMEM, VMEM],
        out_specs=VMEM,
        compiler_params=PARAMS,
        cost_estimate=cost(parts.size, 2**20),
        name="last_sum",
    )(parts, level)


def step(
    group_latents,
    slot_ids,
    slot_embed,
    merge_latents,
    query_weight,
    key_weight,
    value_weight,
    output_weight,
    global_latents,
    decode_query,
    decode_key,
    decode_value,
    decode_output,
):
    inner = lax.axis_size(INNER)
    length, width = merge_latents.shape
    rows = length // inner

    own_rows = lax.dynamic_slice_in_dim(merge_latents, lax.axis_index(INNER) * rows, rows, 0)

    keyed, pack = prepare(
        slot_ids, group_latents, slot_embed, merge_latents, query_weight, key_weight, value_weight
    )
    pack_two = partner(pack, "x", 2)
    keyed_three = partner(keyed, "z", 3)
    outer_block = all_from(global_latents, INNER)
    pack_three = partner(pack, "x", 3)
    keyed_two = partner(keyed, "z", 2)
    pack_one = partner(pack, "x", 1)
    keyed_one = partner(keyed, "z", 1)
    parts = attend_part(
        [keyed, keyed_one, keyed_two, keyed_three],
        [pack, pack_one, pack_two, pack_three],
    )
    parts = exchange(parts, "x")

    pairs = decode_pairs(outer_block, decode_key, decode_value)
    for axis, step_size in (("h", 1), ("h", 3), ("y", 1), ("y", 3)):
        if lax.axis_size(axis) > step_size:
            pairs = jnp.concatenate([pairs, partner(pairs, axis, step_size)], axis=0)
    other = partner(pairs, "c", 1)

    partial = join_and_project(parts, output_weight)
    arrived = exchange(partial.reshape(inner, rows, width), INNER)
    level_two, copies = sum_and_norm(arrived, own_rows)
    normed = exchange(copies, INNER).reshape(length, width)

    query_five = dot(normed, decode_query, ((1,), (0,))).astype(BF16)
    pairs = jnp.concatenate([pairs, other], axis=0)
    scores = dot(pairs[:, :HEAD], query_five, ((1,), (1,))) * SCALE
    top = jnp.max(scores, axis=0, keepdims=True)
    weights = jnp.exp(scores - top)
    total = jnp.sum(weights, axis=0, keepdims=True)
    weights = weights.astype(BF16)
    mixed_five = (dot(pairs[:, HEAD:], weights, ((0,), (0,))) / total).astype(BF16)
    partial = dot(mixed_five, decode_output, ((0,), (0,))).astype(BF16)
    arrived = exchange(partial.reshape(inner, rows, width), INNER)
    return last_sum(arrived, level_two)


def solution(mesh):
    outer, inner = mesh.shape["outer"], mesh.shape["inner"]
    finer = Mesh(mesh.devices.reshape(outer // 8, 4, 2, inner // 4, 4), AXES)
    placed = (
        P(ALL, None),
        P(OUTER, INNER),
        P(),
        P(),
        P(None, INNER),
        P(None, INNER),
        P(None, INNER),
        P(INNER, None),
        P(ALL, None),
        P(None, INNER),
        P(None, INNER),
        P(None, INNER),
        P(INNER, None),
    )
    return jax.shard_map(step, mesh=finer, in_specs=placed, out_specs=P(ALL, None), check_vma=False)
```
